256 devices in a mesh: wav: 32 (over y, x, core), lev: 8 (over z).
Axes of the slice: x: 4, y: 4, z: 8, core: 2. Of those that a mesh axis runs over, the one named last changes fastest.
Arguments:
- spectral: bfloat16 [224, 401, 1024], P('wav', None, 'lev'), may hold values from -0.1796875 to 0.1796875
- legendre: bfloat16 [224, 401, 256], P('wav', None, 'lev'), may hold values from -0.4375 to 0.4375
- wave_pair: int32 [224], replicated, may hold values from -1 to 199, as said below
- lat_slot: int32 [256], replicated, may hold values from 0 to 799, as said below
Outputs:
- gridded: bfloat16 [256, 512, 1616], P('wav', 'lev')
The draws below stay inside these ranges and needn't reach their ends.
Inputs may be any that keep to these rules, and one draw needn't show every extreme that they name: `wave_pair`: each pair number 0 to 199 appears exactly once; all other entries are -1. `lat_slot`: the entries are distinct latitudes.
All inputs are finite; a program needn't handle non-finite values.
Results may differ from the reference program's by a relative error of at most 0.0055.
Values may be sent and summed in bfloat16 or wider, within the bound.
No kernel may reach another device: no remote copies, remote signals or barrier semaphores. Data moves between devices by JAX's collectives and lax.ppermute only.
A program may use at most 64 MiB of HBM per device.

```python
import math
import jax
import jax.numpy as jnp
from jax import lax

WAVES = 400
NLAT = 800
PAIRS = 200
FOLD = 401
WSLOTS = 224
NROWS = 256
LAYERS = 512


def draw_wave_pair(key, part):
    order = jax.random.permutation(jax.random.fold_in(key, 11), WSLOTS)
    return jnp.where(order < PAIRS, order, -1).astype(jnp.int32)


def draw_lat_slot(key, part):
    order = jax.random.permutation(jax.random.fold_in(key, 13), NLAT)
    return order[:NROWS].astype(jnp.int32)


def levels(own_key, extent, shards, least, high):
    gain = 1.0
    for dim, parts in shards:
        heights = jax.random.uniform(jax.random.fold_in(jax.random.fold_in(own_key, 6), dim), (parts,), jnp.float32, least / len(shards), high / len(shards))
        gain = gain * jnp.repeat(jnp.exp(heights), extent[dim] // parts).reshape((-1,) + (1,) * (len(extent) - 1 - dim))
    return gain


def noise(stream_key, shape, scale, bound, pieces=(), kind=jnp.bfloat16):
    entries = scale * jax.random.normal(stream_key, shape, jnp.float32)
    if pieces:
        entries = entries * levels(stream_key, shape, pieces, -0.22, 0.18)
    return jnp.clip(entries, -bound, bound).astype(kind)


def setup_inputs(seed: int = 0) -> dict:
    seeds = jax.random.split(jax.random.key(seed), 5)
    spectral = noise(seeds[0], (WSLOTS, FOLD, 2 * LAYERS), 0.03, 0.1796875, ((0, 32), (2, 8)))
    legendre = noise(seeds[1], (WSLOTS, FOLD, NROWS), (WAVES // 2) ** -0.5, 0.4375, ((0, 32), (2, 8)))
    wave_pair = draw_wave_pair(jax.random.fold_in(seeds[4], 71), 0)
    lat_slot = draw_lat_slot(jax.random.fold_in(seeds[4], 71), 0)
    return {"spectral": spectral, "legendre": legendre, "wave_pair": wave_pair, "lat_slot": lat_slot}


def fold_masks(pair_ids, fold_count, wave_count):
    fold_rows = jnp.arange(fold_count, dtype=jnp.int32)
    filled = pair_ids >= 0
    border = wave_count - pair_ids
    lower = filled[:, None] & (fold_rows[None, :] < border[:, None])
    upper = filled[:, None] & (fold_rows[None, :] >= border[:, None])
    return jnp.stack([lower, upper], axis=1)


def trig_parts(wave_numbers, steps, counts_b):
    residue = (wave_numbers[None, None] * steps[None, :, None, None]) % counts_b
    angles = residue.astype(jnp.float32) * (2.0 * math.pi) / counts_b.astype(jnp.float32)
    return jnp.cos(angles), jnp.sin(angles)


def synthesis_table(pair_ids, row_lats, lat_count, lon_width, wave_count):
    filled = pair_ids >= 0
    wave_numbers = jnp.stack([pair_ids, wave_count - 1 - pair_ids], axis=1)
    lon_count = 20 + 4 * jnp.minimum(row_lats, lat_count - 1 - row_lats)
    highest = jnp.minimum(wave_count - 1, (lon_count - 1) // 2)
    counts_b = lon_count[:, None, None, None]
    coarse_count = (lon_width + 63) // 64
    coarse_steps = jnp.arange(coarse_count, dtype=jnp.int32) * 64
    fine_steps = jnp.arange(64, dtype=jnp.int32)
    cos_coarse, sin_coarse = trig_parts(wave_numbers, coarse_steps, counts_b)
    cos_fine, sin_fine = trig_parts(wave_numbers, fine_steps, counts_b)
    cos_all = cos_coarse[:, :, None] * cos_fine[:, None] - sin_coarse[:, :, None] * sin_fine[:, None]
    sin_all = sin_coarse[:, :, None] * cos_fine[:, None] + cos_coarse[:, :, None] * sin_fine[:, None]
    row_total = row_lats.shape[0]
    cos_all = cos_all.reshape(row_total, coarse_count * 64, wave_numbers.shape[0], 2)[:, :lon_width]
    sin_all = sin_all.reshape(row_total, coarse_count * 64, wave_numbers.shape[0], 2)[:, :lon_width]
    columns = jnp.arange(lon_width, dtype=jnp.int32)
    valid = filled[None, None, :, None] & (wave_numbers[None, None] <= highest[:, None, None, None]) & (columns[None, :, None, None] < counts_b)
    factor = jnp.where(wave_numbers == 0, 1.0, 2.0).astype(jnp.float32)[None, None]
    real_part = jnp.where(valid, factor * cos_all, 0.0)
    imag_part = jnp.where(valid, -factor * sin_all, 0.0)
    return jnp.stack([real_part, imag_part], axis=-1).astype(jnp.bfloat16)


def reference(spectral, legendre, wave_pair, lat_slot):
    fold_count = spectral.shape[1]
    wave_count = fold_count - 1
    lat_count = NLAT
    lon_width = 2 * lat_count + 16
    layer_count = spectral.shape[2] // 2
    row_total = lat_slot.shape[0]
    half_masks = fold_masks(wave_pair, fold_count, wave_count)
    paired = spectral.reshape(spectral.shape[0], fold_count, layer_count, 2)

    def per_slot(args):
        coefficients, weights, masks_one = args
        masked = jnp.where(masks_one[:, :, None, None], coefficients.astype(jnp.float32)[None], 0.0)
        summed = jnp.einsum("htlc,ta->ahcl", masked, weights.astype(jnp.float32))
        return summed.astype(jnp.bfloat16)

    fourier = lax.map(per_slot, (paired, legendre, half_masks))

    def per_row(args):
        latitude, position = args
        basis = synthesis_table(wave_pair, latitude[None], lat_count, lon_width, wave_count)[0]
        picked = jnp.take(fourier, position, axis=1)
        flat_basis = basis.reshape(lon_width, -1).astype(jnp.float32)
        flat_values = picked.reshape(-1, layer_count).astype(jnp.float32)
        result = jnp.dot(flat_basis, flat_values, preferred_element_type=jnp.float32)
        return result.T.astype(jnp.bfloat16)

    positions = jnp.arange(row_total, dtype=jnp.int32)
    return lax.map(per_row, (lat_slot, positions))
```

```python
import jax
import jax.numpy as jnp
from jax import lax
from jax.experimental import pallas as pl
from jax.experimental.pallas import tpu as pltpu
from jax.sharding import PartitionSpec as P

NLAT = 800
WAVES = 400
FOLD = 401
WIDTH = 1616
SLOTS = 7
ROWS = 8
QBLK = 32
MAIN = 384
REST = FOLD - MAIN
PACKED = SLOTS * MAIN + 128
KEEP = 448
KP = 512
FINE = 256
COARSE = 7

COS = (1.0, -19.739208221435547, 64.93938446044922, -85.45662689208984, 60.24171447753906,
       -26.402057647705078, 7.7920684814453125, -1.4433850049972534)
SIN = (6.2831854820251465, -41.34170150756836, 81.6051025390625, -76.70254516601562,
       42.02196502685547, -14.884664535522461, 3.2164907455444336)


def horner(coefs, v):
    total = jnp.full_like(v, coefs[-1])
    for c in coefs[-2::-1]:
        total = total * v + c
    return total


def cos_sin(x, n, inv):
    r = x - jnp.floor(x * inv + 0.5) * n
    u = r * inv
    v = u * u
    return horner(COS, v), u * horner(SIN, v)


def pack_kernel(leg, out, scr):
    total = jnp.zeros((QBLK, 128), jnp.float32)
    scr[...] = total
    for s in range(SLOTS):
        out[:, MAIN * s : MAIN * (s + 1)] = leg[s, :, 0:MAIN]
        scr[:, 0:REST] = leg[s, :, MAIN:FOLD].astype(jnp.float32)
        tail = scr[...]
        total = total + (pltpu.roll(tail, REST * s, 1) if s else tail)
    out[:, SLOTS * MAIN : PACKED] = total.astype(jnp.bfloat16)


def mask_kernel(pairs, spec, out, scr):
    t_main = lax.broadcasted_iota(jnp.int32, (MAIN, 128), 0)
    t_rest = lax.broadcasted_iota(jnp.int32, (128, 128), 0) + MAIN
    for s in range(SLOTS):
        border = WAVES - pairs[s]
        border = jnp.where(pairs[s] >= 0, border, FOLD)
        main = spec[s, 0:MAIN, :].astype(jnp.float32)
        low = jnp.where(t_main < border, main, 0.0)
        out[s, 0:MAIN, 0:128] = low.astype(jnp.bfloat16)
        out[s, 0:MAIN, 128:256] = (main - low).astype(jnp.bfloat16)
        scr[...] = jnp.zeros((128, 128), jnp.float32)
        scr[REST * s : REST * (s + 1), :] = spec[s, MAIN:FOLD, :].astype(jnp.float32)
        rest = scr[...]
        low = jnp.where(t_rest - REST * s < border, rest, 0.0)
        out[s, MAIN:KP, 0:128] = low.astype(jnp.bfloat16)
        out[s, MAIN:KP, 128:256] = (rest - low).astype(jnp.bfloat16)


def legendre_kernel(place, rhs, x0, p1, m1, p2, m2, p3, m3, p4, m4, out):
    z = place[0]
    for s in range(SLOTS):
        def lhs(ref):
            return jnp.concatenate(
                [ref[:, MAIN * s : MAIN * (s + 1)], ref[:, SLOTS * MAIN : PACKED]], axis=1)
        left = jnp.concatenate([lhs(r) for r in (x0, p1, m1, p2, m2, p3, m3, p4, m4)], axis=0)
        got = jnp.dot(left, rhs[s], preferred_element_type=jnp.float32)
        for i, d in enumerate((0, 1, -1, 2, -2, 3, -3, 4)):
            block = lax.rem(z - d + 8, 8)
            for h in range(2):
                part = got[QBLK * i : QBLK * (i + 1), 128 * h : 128 * (h + 1)]
                out[pl.ds(4 * block, 4), 2 * s + h] = part.reshape(4, ROWS, 128).astype(jnp.bfloat16)


def table_kernel(lats, waves, fine, coarse):
    a = lats[pl.program_id(0)]
    lon = 20 + 4 * jnp.minimum(a, NLAT - 1 - a)
    highest = jnp.minimum(WAVES - 1, (lon - 1) // 2).astype(jnp.float32)
    m = waves[...]
    n = jnp.full((1, KP), lon, jnp.int32).astype(jnp.float32)
    inv = 1.0 / n
    scale = jnp.where((m >= 0.0) & (m <= highest), jnp.where(m == 0.0, 1.0, 2.0), 0.0)

    def at(step, count):
        j = step * lax.broadcasted_iota(jnp.int32, (count, KP), 0)
        return cos_sin(j.astype(jnp.float32) * m, n, inv)

    cos_b, sin_b = at(1, 32)
    cos_a, sin_a = at(32, 8)
    cos_a = cos_a * scale
    sin_a = sin_a * scale
    for i in range(FINE // 32):
        ca = cos_a[i : i + 1, :]
        sa = sin_a[i : i + 1, :]
        rows = slice(32 * i, 32 * (i + 1))
        fine[0, rows, 0:KP] = (ca * cos_b - sa * sin_b).astype(jnp.bfloat16)
        fine[0, rows, KP : 2 * KP] = (-(sa * cos_b + ca * sin_b)).astype(jnp.bfloat16)
    cos_c, sin_c = at(FINE, 8)
    coarse[0, :, 0:KP] = cos_c
    coarse[0, :, KP : 2 * KP] = sin_c


def synth_kernel(lats, recv, fine, coarse, out, scr, lhs):
    q = pl.program_id(0)
    a = lats[q]
    lon = 20 + 4 * jnp.minimum(a, NLAT - 1 - a)

    @pl.when(q == 0)
    def _():
        for i in range(7):
            scr[512 * i : 512 * (i + 1), :] = (
                recv[64 * i : 64 * (i + 1)].astype(jnp.float32).reshape(512, 128))
        scr[KEEP * ROWS : KP * ROWS, :] = jnp.zeros(((KP - KEEP) * ROWS, 128), jnp.float32)

    row = lax.broadcasted_iota(jnp.int32, (128, 128), 0)
    col = lax.broadcasted_iota(jnp.int32, (128, 128), 1)
    source = jnp.where(row < 64, 2 * row, 2 * row - 127)
    perm = jnp.where(col == source, 1.0, 0.0).astype(jnp.bfloat16)
    values = scr[pl.ds(q, KP, stride=ROWS), :].astype(jnp.bfloat16)
    nt = (((1,), (1,)), ((), ()))
    turned = lax.dot_general(perm, values, nt, preferred_element_type=jnp.float32)
    re = turned[0:64, :]
    im = turned[64:128, :]
    for jc in range(COARSE):
        cc = coarse[0, jc : jc + 1, 0:KP]
        sc = coarse[0, jc : jc + 1, KP : 2 * KP]
        lhs[64 * jc : 64 * (jc + 1), 0:KP] = (cc * re - sc * im).astype(jnp.bfloat16)
        lhs[64 * jc : 64 * (jc + 1), KP : 2 * KP] = (sc * re + cc * im).astype(jnp.bfloat16)
    result = lax.dot_general(lhs[...], fine[0], nt, preferred_element_type=jnp.float32)
    column = lax.broadcasted_iota(jnp.int32, (64, FINE), 1)
    for jc in range(COARSE):
        width = min(FINE, WIDTH - FINE * jc)
        block = result[64 * jc : 64 * (jc + 1), :]
        block = jnp.where(column < lon - FINE * jc, block, 0.0).astype(jnp.bfloat16)
        out[0, :, FINE * jc : FINE * jc + width] = block[:, 0:width]


def cost(flops, moved):
    return pl.CostEstimate(flops=flops, transcendentals=0, bytes_accessed=moved)


def gather_pieces(x):
    def shift(v, d):
        return lax.ppermute(v, "lev", [(i, (i + d) % 8) for i in range(8)])

    p1, m1 = shift(x, 1), shift(x, -1)
    p2, m2 = shift(x, 2), shift(x, -2)
    p3, m3 = shift(p2, 1), shift(m2, -1)
    half = QBLK // 2
    p4, m4 = shift(p2[:half], 2), shift(m2[half:], -2)
    return x, p1, m1, p2, m2, p3, m3, p4, m4


def on_device(spectral, legendre, wave_pair, lat_slot):
    bf16, f32 = jnp.bfloat16, jnp.float32
    smem = pl.BlockSpec(memory_space=pltpu.SMEM)
    vmem = pl.BlockSpec(memory_space=pltpu.VMEM)
    z = lax.axis_index("lev").astype(jnp.int32)
    w = lax.axis_index("wav").astype(jnp.int32)
    own_pairs = lax.dynamic_slice_in_dim(wave_pair, w * SLOTS, SLOTS)
    own_lats = lax.dynamic_slice_in_dim(lat_slot, w * ROWS, ROWS)
    waves = jnp.stack([wave_pair, WAVES - 1 - wave_pair], axis=1)
    waves = jnp.where(wave_pair[:, None] >= 0, waves, -1).reshape(1, KEEP)
    waves = jnp.pad(waves, ((0, 0), (0, KP - KEEP)), constant_values=-1).astype(f32)

    packed = pl.pallas_call(
        pack_kernel,
        out_shape=jax.ShapeDtypeStruct((QBLK, PACKED), bf16),
        in_specs=[vmem], out_specs=vmem,
        scratch_shapes=[pltpu.VMEM((QBLK, 128), f32)],
        name="pack",
    )(jnp.transpose(legendre, (0, 2, 1)))
    pieces = gather_pieces(packed)

    rhs = pl.pallas_call(
        mask_kernel,
        out_shape=jax.ShapeDtypeStruct((SLOTS, KP, 256), bf16),
        in_specs=[smem, vmem], out_specs=vmem,
        scratch_shapes=[pltpu.VMEM((128, 128), f32)],
        cost_estimate=cost(2_000_000_000, 2_500_000),
        name="mask",
    )(own_pairs, spectral)

    fine, coarse = pl.pallas_call(
        table_kernel,
        out_shape=(jax.ShapeDtypeStruct((ROWS, FINE, 2 * KP), bf16),
                   jax.ShapeDtypeStruct((ROWS, 8, 2 * KP), f32)),
        grid_spec=pltpu.PrefetchScalarGridSpec(
            num_scalar_prefetch=1, grid=(ROWS,),
            in_specs=[pl.BlockSpec((1, KP), lambda q, lats: (0, 0))],
            out_specs=(pl.BlockSpec((1, FINE, 2 * KP), lambda q, lats: (q, 0, 0)),
                       pl.BlockSpec((1, 8, 2 * KP), lambda q, lats: (q, 0, 0)))),
        cost_estimate=cost(4_000_000_000, 4_500_000),
        name="tables",
    )(own_lats, waves)

    fourier = pl.pallas_call(
        legendre_kernel,
        out_shape=jax.ShapeDtypeStruct((32, 2 * SLOTS, ROWS, 128), bf16),
        in_specs=[smem] + [vmem] * 10, out_specs=vmem,
        cost_estimate=cost(2 * 256 * 512 * 256 * SLOTS, 4_000_000),
        name="legendre",
    )(z.reshape(1), rhs, *pieces)

    received = lax.all_to_all(fourier, "wav", split_axis=0, concat_axis=0, tiled=True)

    return pl.pallas_call(
        synth_kernel,
        out_shape=jax.ShapeDtypeStruct((ROWS, 64, WIDTH), bf16),
        grid_spec=pltpu.PrefetchScalarGridSpec(
            num_scalar_prefetch=1, grid=(ROWS,),
            in_specs=[pl.BlockSpec((KEEP, ROWS, 128), lambda q, lats: (0, 0, 0)),
                      pl.BlockSpec((1, FINE, 2 * KP), lambda q, lats: (q, 0, 0)),
                      pl.BlockSpec((1, 8, 2 * KP), lambda q, lats: (q, 0, 0))],
            out_specs=pl.BlockSpec((1, 64, WIDTH), lambda q, lats: (q, 0, 0)),
            scratch_shapes=[pltpu.VMEM((KP * ROWS, 128), f32),
                            pltpu.VMEM((64 * COARSE, 2 * KP), bf16)]),
        cost_estimate=cost(2 * 448 * 1024 * 256 * ROWS, 18_000_000),
        name="synth",
    )(own_lats, received.reshape(KEEP, ROWS, 128), fine, coarse)


def solution(mesh):
    return jax.shard_map(
        on_device,
        mesh=mesh,
        in_specs=(P("wav", None, "lev"), P("wav", None, "lev"), P(), P()),
        out_specs=P("wav", "lev", None),
        check_vma=False,
    )
```

```python
import jax
import jax.numpy as jnp
from jax import lax
from jax.experimental import pallas as pl
from jax.experimental.pallas import tpu as pltpu
from jax.sharding import PartitionSpec as P

NLAT = 800
WAVES = 400
FOLD = 401
WIDTH = 1616
SLOTS = 7
ROWS = 8
QBLK = 32
MAIN = 384
REST = FOLD - MAIN
PACKED = SLOTS * MAIN + 128
KEEP = 448
KP = 512
FINE = 256
COARSE = 7

COS = (1.0, -19.739208221435547, 64.93938446044922, -85.45662689208984, 60.24171447753906,
       -26.402057647705078, 7.7920684814453125, -1.4433850049972534)
SIN = (6.2831854820251465, -41.34170150756836, 81.6051025390625, -76.70254516601562,
       42.02196502685547, -14.884664535522461, 3.2164907455444336)


def horner(coefs, v):
    total = jnp.full_like(v, coefs[-1])
    for c in coefs[-2::-1]:
        total = total * v + c
    return total


def cos_sin(x, n, inv):
    r = x - jnp.floor(x * inv + 0.5) * n
    u = r * inv
    v = u * u
    return horner(COS, v), u * horner(SIN, v)


def pack_kernel(leg, out, scr):
    total = jnp.zeros((QBLK, 128), jnp.float32)
    scr[...] = total
    for s in range(SLOTS):
        out[:, MAIN * s : MAIN * (s + 1)] = leg[s, :, 0:MAIN]
        scr[:, 0:REST] = leg[s, :, MAIN:FOLD].astype(jnp.float32)
        tail = scr[...]
        total = total + (pltpu.roll(tail, REST * s, 1) if s else tail)
    out[:, SLOTS * MAIN : PACKED] = total.astype(jnp.bfloat16)


def mask_kernel(pairs, spec, out, scr):
    t_main = lax.broadcasted_iota(jnp.int32, (MAIN, 128), 0)
    t_rest = lax.broadcasted_iota(jnp.int32, (128, 128), 0) + MAIN
    for s in range(SLOTS):
        border = WAVES - pairs[s]
        border = jnp.where(pairs[s] >= 0, border, FOLD)
        main = spec[s, 0:MAIN, :].astype(jnp.float32)
        low = jnp.where(t_main < border, main, 0.0)
        out[s, 0:MAIN, 0:128] = low.astype(jnp.bfloat16)
        out[s, 0:MAIN, 128:256] = (main - low).astype(jnp.bfloat16)
        scr[...] = jnp.zeros((128, 128), jnp.float32)
        scr[REST * s : REST * (s + 1), :] = spec[s, MAIN:FOLD, :].astype(jnp.float32)
        rest = scr[...]
        low = jnp.where(t_rest - REST * s < border, rest, 0.0)
        out[s, MAIN:KP, 0:128] = low.astype(jnp.bfloat16)
        out[s, MAIN:KP, 128:256] = (rest - low).astype(jnp.bfloat16)


def legendre_kernel(place, rhs, x0, p1, m1, p2, m2, p3, m3, p4, m4, out):
    z = place[0]
    for s in range(SLOTS):
        def lhs(ref):
            return jnp.concatenate(
                [ref[:, MAIN * s : MAIN * (s + 1)], ref[:, SLOTS * MAIN : PACKED]], axis=1)
        left = jnp.concatenate([lhs(r) for r in (x0, p1, m1, p2, m2, p3, m3, p4, m4)], axis=0)
        got = jnp.dot(left, rhs[s], preferred_element_type=jnp.float32)
        for i, d in enumerate((0, 1, -1, 2, -2, 3, -3, 4)):
            block = lax.rem(z - d + 8, 8)
            for h in range(2):
                part = got[QBLK * i : QBLK * (i + 1), 128 * h : 128 * (h + 1)]
                out[pl.ds(4 * block, 4), 2 * s + h] = part.reshape(4, ROWS, 128).astype(jnp.bfloat16)


def table_kernel(lats, waves, fine, coarse):
    m = waves[...]

    def one_row(q, carry):
        a = lats[q]
        lon = 20 + 4 * jnp.minimum(a, NLAT - 1 - a)
        highest = jnp.minimum(WAVES - 1, (lon - 1) // 2).astype(jnp.float32)
        n = jnp.full((1, KP), lon, jnp.int32).astype(jnp.float32)
        inv = 1.0 / n
        scale = jnp.where((m >= 0.0) & (m <= highest), jnp.where(m == 0.0, 1.0, 2.0), 0.0)

        def at(step, count):
            j = step * lax.broadcasted_iota(jnp.int32, (count, KP), 0)
            return cos_sin(j.astype(jnp.float32) * m, n, inv)

        cos_b, sin_b = at(1, 32)
        cos_a, sin_a = at(32, 8)
        cos_a = cos_a * scale
        sin_a = sin_a * scale
        for i in range(FINE // 32):
            ca = cos_a[i : i + 1, :]
            sa = sin_a[i : i + 1, :]
            rows = slice(32 * i, 32 * (i + 1))
            fine[q, rows, 0:KP] = (ca * cos_b - sa * sin_b).astype(jnp.bfloat16)
            fine[q, rows, KP : 2 * KP] = (-(sa * cos_b + ca * sin_b)).astype(jnp.bfloat16)
        cos_c, sin_c = at(FINE, 8)
        coarse[q, :, 0:KP] = cos_c
        coarse[q, :, KP : 2 * KP] = sin_c
        return carry

    lax.fori_loop(0, ROWS, one_row, 0)


def synth_kernel(lats, recv, tables, coarse, out, scr, lhs, rows, fine, sems, in_sems):
    def fetch(q):
        return pltpu.make_async_copy(tables.at[q], fine.at[q], in_sems.at[q])

    for q in range(ROWS):
        fetch(q).start()
    for i in range(7):
        scr[512 * i : 512 * (i + 1), :] = (
            recv[64 * i : 64 * (i + 1)].astype(jnp.float32).reshape(512, 128))
    scr[KEEP * ROWS : KP * ROWS, :] = jnp.zeros(((KP - KEEP) * ROWS, 128), jnp.float32)

    row = lax.broadcasted_iota(jnp.int32, (128, 128), 0)
    col = lax.broadcasted_iota(jnp.int32, (128, 128), 1)
    source = jnp.where(row < 64, 2 * row, 2 * row - 127)
    perm = jnp.where(col == source, 1.0, 0.0).astype(jnp.bfloat16)
    column = lax.broadcasted_iota(jnp.int32, (64, FINE), 1)
    nt = (((1,), (1,)), ((), ()))

    def rotate(q, to):
        values = scr[pl.ds(q, KP, stride=ROWS), :].astype(jnp.bfloat16)
        turned = lax.dot_general(perm, values, nt, preferred_element_type=jnp.float32)
        re = turned[0:64, :]
        im = turned[64:128, :]
        for jc in range(COARSE):
            cc = coarse[q, jc : jc + 1, 0:KP]
            sc = coarse[q, jc : jc + 1, KP : 2 * KP]
            at = slice(64 * jc, 64 * (jc + 1))
            lhs[to, at, 0:KP] = (cc * re - sc * im).astype(jnp.bfloat16)
            lhs[to, at, KP : 2 * KP] = (sc * re + cc * im).astype(jnp.bfloat16)

    def copy(q):
        return pltpu.make_async_copy(rows.at[q], out.at[q], sems.at[q])

    def one_row(q, carry):
        slot = lax.rem(q, 2)
        fetch(q).wait()
        a = lats[q]
        lon = 20 + 4 * jnp.minimum(a, NLAT - 1 - a)
        result = lax.dot_general(lhs[slot], fine[q], nt, preferred_element_type=jnp.float32)
        rotate(jnp.minimum(q + 1, ROWS - 1), 1 - slot)
        for jc in range(COARSE):
            width = min(FINE, WIDTH - FINE * jc)
            block = result[64 * jc : 64 * (jc + 1), :]
            block = jnp.where(column < lon - FINE * jc, block, 0.0).astype(jnp.bfloat16)
            rows[q, :, FINE * jc : FINE * jc + width] = block[:, 0:width]
        copy(q).start()
        return carry

    rotate(0, 0)
    lax.fori_loop(0, ROWS, one_row, 0)
    for q in range(ROWS):
        copy(q).wait()


def cost(flops, moved):
    return pl.CostEstimate(flops=flops, transcendentals=0, bytes_accessed=moved)


def gather_pieces(x):
    def shift(v, d):
        return lax.ppermute(v, "lev", [(i, (i + d) % 8) for i in range(8)])

    p1, m1 = shift(x, 1), shift(x, -1)
    p2, m2 = shift(x, 2), shift(x, -2)
    p3, m3 = shift(p2, 1), shift(m2, -1)
    half = QBLK // 2
    p4, m4 = shift(p2[:half], 2), shift(m2[half:], -2)
    return x, p1, m1, p2, m2, p3, m3, p4, m4


def on_device(spectral, legendre, wave_pair, lat_slot):
    bf16, f32 = jnp.bfloat16, jnp.float32
    smem = pl.BlockSpec(memory_space=pltpu.SMEM)
    vmem = pl.BlockSpec(memory_space=pltpu.VMEM)
    z = lax.axis_index("lev").astype(jnp.int32)
    w = lax.axis_index("wav").astype(jnp.int32)
    own_pairs = lax.dynamic_slice_in_dim(wave_pair, w * SLOTS, SLOTS)
    own_lats = lax.dynamic_slice_in_dim(lat_slot, w * ROWS, ROWS)
    waves = jnp.stack([wave_pair, WAVES - 1 - wave_pair], axis=1)
    waves = jnp.where(wave_pair[:, None] >= 0, waves, -1).reshape(1, KEEP)
    waves = jnp.pad(waves, ((0, 0), (0, KP - KEEP)), constant_values=-1).astype(f32)

    def here(v):
        return pltpu.with_memory_space_constraint(v, pltpu.VMEM)

    def params(mib):
        return pltpu.CompilerParams(vmem_limit_bytes=mib * 2**20)

    packed = pl.pallas_call(
        pack_kernel,
        out_shape=pltpu.VMEM((QBLK, PACKED), bf16),
        in_specs=[vmem], out_specs=vmem,
        scratch_shapes=[pltpu.VMEM((QBLK, 128), f32)],
        compiler_params=params(4),
        name="pack",
    )(jnp.transpose(legendre, (0, 2, 1)))
    pieces = gather_pieces(packed)

    rhs = pl.pallas_call(
        mask_kernel,
        out_shape=pltpu.VMEM((SLOTS, KP, 256), bf16),
        in_specs=[smem, vmem], out_specs=vmem,
        scratch_shapes=[pltpu.VMEM((128, 128), f32)],
        cost_estimate=cost(2_000_000_000, 2_500_000),
        compiler_params=params(6),
        name="mask",
    )(own_pairs, spectral)

    fine, coarse = pl.pallas_call(
        table_kernel,
        out_shape=(pltpu.HBM((ROWS, FINE, 2 * KP), bf16),
                   pltpu.VMEM((ROWS, 8, 2 * KP), f32)),
        in_specs=[smem, vmem], out_specs=(vmem, vmem),
        cost_estimate=cost(4_000_000_000, 4_500_000),
        compiler_params=params(8),
        name="tables",
    )(own_lats, waves)

    fourier = pl.pallas_call(
        legendre_kernel,
        out_shape=pltpu.VMEM((32, 2 * SLOTS, ROWS, 128), bf16),
        in_specs=[smem] + [vmem] * 10, out_specs=vmem,
        cost_estimate=cost(2 * 256 * 512 * 256 * SLOTS, 4_000_000),
        compiler_params=params(12),
        name="legendre",
    )(z.reshape(1), here(rhs), *[here(p) for p in pieces])

    received = lax.all_to_all(fourier, "wav", split_axis=0, concat_axis=0, tiled=True)

    return pl.pallas_call(
        synth_kernel,
        out_shape=jax.ShapeDtypeStruct((ROWS, 64, WIDTH), bf16),
        in_specs=[smem, vmem, pl.BlockSpec(memory_space=pltpu.HBM), vmem],
        out_specs=pl.BlockSpec(memory_space=pltpu.HBM),
        scratch_shapes=[pltpu.VMEM((KP * ROWS, 128), f32),
                        pltpu.VMEM((2, 64 * COARSE, 2 * KP), bf16),
                        pltpu.VMEM((ROWS, 64, WIDTH), bf16),
                        pltpu.VMEM((ROWS, FINE, 2 * KP), bf16),
                        pltpu.SemaphoreType.DMA((ROWS,)),
                        pltpu.SemaphoreType.DMA((ROWS,))],
        cost_estimate=cost(2 * 448 * 1024 * 256 * ROWS, 18_000_000),
        compiler_params=params(16),
        name="synth",
    )(own_lats, here(received.reshape(KEEP, ROWS, 128)),
      pltpu.with_memory_space_constraint(fine, pltpu.HBM), here(coarse))


def solution(mesh):
    return jax.shard_map(
        on_device,
        mesh=mesh,
        in_specs=(P("wav", None, "lev"), P("wav", None, "lev"), P(), P()),
        out_specs=P("wav", "lev", None),
        check_vma=False,
    )
```

```python
import jax
import jax.numpy as jnp
from jax import lax
from jax.experimental import pallas as pl
from jax.experimental.pallas import tpu as pltpu
from jax.sharding import PartitionSpec as P

NLAT = 800
WAVES = 400
FOLD = 401
WIDTH = 1616
SLOTS = 7
ROWS = 8
QBLK = 32
MAIN = 384
REST = FOLD - MAIN
PACKED = SLOTS * MAIN + 128
KEEP = 448
KP = 512
FINE = 256
COARSE = 7

COS = (1.0, -19.739208221435547, 64.93938446044922, -85.45662689208984, 60.24171447753906,
       -26.402057647705078, 7.7920684814453125, -1.4433850049972534)
SIN = (6.2831854820251465, -41.34170150756836, 81.6051025390625, -76.70254516601562,
       42.02196502685547, -14.884664535522461, 3.2164907455444336)


def horner(coefs, v):
    total = jnp.full_like(v, coefs[-1])
    for c in coefs[-2::-1]:
        total = total * v + c
    return total


def cos_sin(x, n, inv):
    r = x - jnp.floor(x * inv + 0.5) * n
    u = r * inv
    v = u * u
    return horner(COS, v), u * horner(SIN, v)


def pack_kernel(leg, out, scr):
    total = jnp.zeros((QBLK, 128), jnp.float32)
    scr[...] = total
    for s in range(SLOTS):
        out[:, MAIN * s : MAIN * (s + 1)] = leg[s, :, 0:MAIN]
        scr[:, 0:REST] = leg[s, :, MAIN:FOLD].astype(jnp.float32)
        tail = scr[...]
        total = total + (pltpu.roll(tail, REST * s, 1) if s else tail)
    out[:, SLOTS * MAIN : PACKED] = total.astype(jnp.bfloat16)


def mask_kernel(pairs, spec, out, scr):
    t_main = lax.broadcasted_iota(jnp.int32, (MAIN, 128), 0)
    t_rest = lax.broadcasted_iota(jnp.int32, (128, 128), 0) + MAIN
    for s in range(SLOTS):
        border = WAVES - pairs[s]
        border = jnp.where(pairs[s] >= 0, border, FOLD)
        main = spec[s, 0:MAIN, :].astype(jnp.float32)
        low = jnp.where(t_main < border, main, 0.0)
        out[s, 0:MAIN, 0:128] = low.astype(jnp.bfloat16)
        out[s, 0:MAIN, 128:256] = (main - low).astype(jnp.bfloat16)
        scr[...] = jnp.zeros((128, 128), jnp.float32)
        scr[REST * s : REST * (s + 1), :] = spec[s, MAIN:FOLD, :].astype(jnp.float32)
        rest = scr[...]
        low = jnp.where(t_rest - REST * s < border, rest, 0.0)
        out[s, MAIN:KP, 0:128] = low.astype(jnp.bfloat16)
        out[s, MAIN:KP, 128:256] = (rest - low).astype(jnp.bfloat16)


def legendre_kernel(place, rhs, x0, p1, m1, p2, m2, p3, m3, p4, m4, out):
    z = place[0]
    for s in range(SLOTS):
        def lhs(ref):
            return jnp.concatenate(
                [ref[:, MAIN * s : MAIN * (s + 1)], ref[:, SLOTS * MAIN : PACKED]], axis=1)
        left = jnp.concatenate([lhs(r) for r in (x0, p1, m1, p2, m2, p3, m3, p4, m4)], axis=0)
        got = jnp.dot(left, rhs[s], preferred_element_type=jnp.float32)
        for i, d in enumerate((0, 1, -1, 2, -2, 3, -3, 4)):
            block = lax.rem(z - d + 8, 8)
            for h in range(2):
                part = got[QBLK * i : QBLK * (i + 1), 128 * h : 128 * (h + 1)]
                out[pl.ds(4 * block, 4), 2 * s + h] = part.reshape(4, ROWS, 128).astype(jnp.bfloat16)


def table_kernel(lats, waves, fine, coarse):
    m = waves[...]

    def one_row(q, carry):
        a = lats[q]
        lon = 20 + 4 * jnp.minimum(a, NLAT - 1 - a)
        highest = jnp.minimum(WAVES - 1, (lon - 1) // 2).astype(jnp.float32)
        n = jnp.full((1, KP), lon, jnp.int32).astype(jnp.float32)
        inv = 1.0 / n
        scale = jnp.where((m >= 0.0) & (m <= highest), jnp.where(m == 0.0, 1.0, 2.0), 0.0)

        def at(step, count):
            j = step * lax.broadcasted_iota(jnp.int32, (count, KP), 0)
            return cos_sin(j.astype(jnp.float32) * m, n, inv)

        cos_b, sin_b = at(1, 32)
        cos_a, sin_a = at(32, 8)
        cos_a = cos_a * scale
        sin_a = sin_a * scale
        for i in range(FINE // 32):
            ca = cos_a[i : i + 1, :]
            sa = sin_a[i : i + 1, :]
            rows = slice(32 * i, 32 * (i + 1))
            fine[q, rows, 0:KP] = (ca * cos_b - sa * sin_b).astype(jnp.bfloat16)
            fine[q, rows, KP : 2 * KP] = (-(sa * cos_b + ca * sin_b)).astype(jnp.bfloat16)
        step = lax.broadcasted_iota(jnp.int32, (8, KP), 0)
        step = FINE * jnp.where(step == 0, 3, step)
        cos_c, sin_c = cos_sin(step.astype(jnp.float32) * m, n, inv)
        coarse[q, :, 0:KP] = cos_c
        coarse[q, :, KP : 2 * KP] = sin_c
        return carry

    lax.fori_loop(0, ROWS, one_row, 0)


def synth_kernel(lats, recv, tables, coarse, out, scr, turn_a, turn_b, lhs_a, lhs_b, rows,
                 fine, sems, in_sems):
    def fetch(q):
        return pltpu.make_async_copy(tables.at[q], fine.at[q], in_sems.at[q])

    for q in range(ROWS):
        fetch(q).start()
    for i in range(7):
        scr[512 * i : 512 * (i + 1), :] = (
            recv[64 * i : 64 * (i + 1)].astype(jnp.float32).reshape(512, 128))
    scr[KEEP * ROWS : KP * ROWS, :] = jnp.zeros(((KP - KEEP) * ROWS, 128), jnp.float32)

    row = lax.broadcasted_iota(jnp.int32, (128, 128), 0)
    col = lax.broadcasted_iota(jnp.int32, (128, 128), 1)
    source = jnp.where(row < 64, 2 * row, 2 * row - 127)
    perm = jnp.where(col == source, 1.0, 0.0).astype(jnp.bfloat16)
    column = lax.broadcasted_iota(jnp.int32, (64, FINE), 1)
    nt = (((1,), (1,)), ((), ()))

    def turn_row(q, turn):
        values = scr[pl.ds(q, KP, stride=ROWS), :].astype(jnp.bfloat16)
        turn[...] = lax.dot_general(perm, values, nt, preferred_element_type=jnp.float32)

    def rotate(q, turn, lhs):
        for lane in range(0, KP, 128):
            here = slice(lane, lane + 128)
            beside = slice(KP + lane, KP + lane + 128)
            for g in range(0, 64, 16):
                def put(block, left, right):
                    at = slice(64 * block + g, 64 * block + g + 16)
                    lhs[at, here] = left.astype(jnp.bfloat16)
                    lhs[at, beside] = right.astype(jnp.bfloat16)

                re = turn[g : g + 16, here]
                im = turn[64 + g : 80 + g, here]
                cc = coarse[q, 0:1, here]
                sc = coarse[q, 0:1, beside]
                re, im = cc * re - sc * im, sc * re + cc * im
                put(0, re, im)
                for step in range(1, 4):
                    cc = coarse[q, step : step + 1, here]
                    sc = coarse[q, step : step + 1, beside]
                    put(2 * step - 1, cc * re, cc * im)
                    put(2 * step, sc * im, -sc * re)

    def copy(q):
        return pltpu.make_async_copy(rows.at[q], out.at[q], sems.at[q])

    def one_row(q, lhs, other, turn, spare):
        fetch(q).wait()
        a = lats[q]
        lon = 20 + 4 * jnp.minimum(a, NLAT - 1 - a)
        result = lax.dot_general(lhs[...], fine[q], nt, preferred_element_type=jnp.float32)
        rotate(jnp.minimum(q + 1, ROWS - 1), turn, other)
        turn_row(jnp.minimum(q + 2, ROWS - 1), spare)

        def put(jc, block):
            width = min(FINE, WIDTH - FINE * jc)
            block = jnp.where(column < lon - FINE * jc, block, 0.0).astype(jnp.bfloat16)
            rows[q, :, FINE * jc : FINE * jc + width] = block[:, 0:width]

        put(3, result[0:64, :])
        for step in range(1, 4):
            even = result[128 * step - 64 : 128 * step, :]
            odd = result[128 * step : 128 * step + 64, :]
            put(3 + step, even - odd)
            put(3 - step, even + odd)
        copy(q).start()

    def two_rows(i, carry):
        one_row(2 * i, lhs_a, lhs_b, turn_b, turn_a)
        one_row(2 * i + 1, lhs_b, lhs_a, turn_a, turn_b)
        return carry

    turn_row(0, turn_a)
    turn_row(1, turn_b)
    rotate(0, turn_a, lhs_a)
    lax.fori_loop(0, ROWS // 2, two_rows, 0)
    for q in range(ROWS):
        copy(q).wait()


def cost(flops, moved):
    return pl.CostEstimate(flops=flops, transcendentals=0, bytes_accessed=moved)


def gather_pieces(x):
    def shift(v, d):
        return lax.ppermute(v, "lev", [(i, (i + d) % 8) for i in range(8)])

    p1, m1 = shift(x, 1), shift(x, -1)
    p2, m2 = shift(x, 2), shift(x, -2)
    p3, m3 = shift(p2, 1), shift(m2, -1)
    half = QBLK // 2
    p4, m4 = shift(p2[:half], 2), shift(m2[half:], -2)
    return x, p1, m1, p2, m2, p3, m3, p4, m4


def on_device(spectral, legendre, wave_pair, lat_slot):
    bf16, f32 = jnp.bfloat16, jnp.float32
    smem = pl.BlockSpec(memory_space=pltpu.SMEM)
    vmem = pl.BlockSpec(memory_space=pltpu.VMEM)
    z = lax.axis_index("lev").astype(jnp.int32)
    w = lax.axis_index("wav").astype(jnp.int32)
    own_pairs = lax.dynamic_slice_in_dim(wave_pair, w * SLOTS, SLOTS)
    own_lats = lax.dynamic_slice_in_dim(lat_slot, w * ROWS, ROWS)
    waves = jnp.stack([wave_pair, WAVES - 1 - wave_pair], axis=1)
    waves = jnp.where(wave_pair[:, None] >= 0, waves, -1).reshape(1, KEEP)
    waves = jnp.pad(waves, ((0, 0), (0, KP - KEEP)), constant_values=-1).astype(f32)

    def here(v):
        return pltpu.with_memory_space_constraint(v, pltpu.VMEM)

    def params(mib):
        return pltpu.CompilerParams(vmem_limit_bytes=mib * 2**20)

    packed = pl.pallas_call(
        pack_kernel,
        out_shape=pltpu.VMEM((QBLK, PACKED), bf16),
        in_specs=[vmem], out_specs=vmem,
        scratch_shapes=[pltpu.VMEM((QBLK, 128), f32)],
        compiler_params=params(4),
        name="pack",
    )(jnp.transpose(legendre, (0, 2, 1)))
    pieces = gather_pieces(packed)

    rhs = pl.pallas_call(
        mask_kernel,
        out_shape=pltpu.VMEM((SLOTS, KP, 256), bf16),
        in_specs=[smem, vmem], out_specs=vmem,
        scratch_shapes=[pltpu.VMEM((128, 128), f32)],
        cost_estimate=cost(2_000_000_000, 2_500_000),
        compiler_params=params(6),
        name="mask",
    )(own_pairs, spectral)

    fine, coarse = pl.pallas_call(
        table_kernel,
        out_shape=(pltpu.HBM((ROWS, FINE, 2 * KP), bf16),
                   pltpu.VMEM((ROWS, 8, 2 * KP), f32)),
        in_specs=[smem, vmem], out_specs=(vmem, vmem),
        cost_estimate=cost(4_000_000_000, 4_500_000),
        compiler_params=params(8),
        name="tables",
    )(own_lats, waves)

    fourier = pl.pallas_call(
        legendre_kernel,
        out_shape=pltpu.VMEM((32, 2 * SLOTS, ROWS, 128), bf16),
        in_specs=[smem] + [vmem] * 10, out_specs=vmem,
        cost_estimate=cost(2 * 256 * 512 * 256 * SLOTS, 4_000_000),
        compiler_params=params(12),
        name="legendre",
    )(z.reshape(1), here(rhs), *[here(p) for p in pieces])

    received = lax.all_to_all(fourier, "wav", split_axis=0, concat_axis=0, tiled=True)

    return pl.pallas_call(
        synth_kernel,
        out_shape=jax.ShapeDtypeStruct((ROWS, 64, WIDTH), bf16),
        in_specs=[smem, vmem, pl.BlockSpec(memory_space=pltpu.HBM), vmem],
        out_specs=pl.BlockSpec(memory_space=pltpu.HBM),
        scratch_shapes=[pltpu.VMEM((KP * ROWS, 128), f32),
                        pltpu.VMEM((128, KP), f32),
                        pltpu.VMEM((128, KP), f32),
                        pltpu.VMEM((64 * COARSE, 2 * KP), bf16),
                        pltpu.VMEM((64 * COARSE, 2 * KP), bf16),
                        pltpu.VMEM((ROWS, 64, WIDTH), bf16),
                        pltpu.VMEM((ROWS, FINE, 2 * KP), bf16),
                        pltpu.SemaphoreType.DMA((ROWS,)),
                        pltpu.SemaphoreType.DMA((ROWS,))],
        cost_estimate=cost(2 * 448 * 1024 * 256 * ROWS, 18_000_000),
        compiler_params=params(16),
        name="synth",
    )(own_lats, here(received.reshape(KEEP, ROWS, 128)),
      pltpu.with_memory_space_constraint(fine, pltpu.HBM), here(coarse))


def solution(mesh):
    return jax.shard_map(
        on_device,
        mesh=mesh,
        in_specs=(P("wav", None, "lev"), P("wav", None, "lev"), P(), P()),
        out_specs=P("wav", "lev", None),
        check_vma=False,
    )
```

```python
import jax
import jax.numpy as jnp
from jax import lax
from jax.experimental import pallas as pl
from jax.experimental.pallas import tpu as pltpu
from jax.sharding import PartitionSpec as P

NLAT = 800
WAVES = 400
FOLD = 401
WIDTH = 1616
SLOTS = 7
ROWS = 8
QBLK = 32
MAIN = 384
REST = FOLD - MAIN
PACKED = SLOTS * MAIN + 128
KEEP = 448
KP = 512
FINE = 256
COARSE = 7

COS = (1.0, -19.739208221435547, 64.93938446044922, -85.45662689208984, 60.24171447753906,
       -26.402057647705078, 7.7920684814453125, -1.4433850049972534)
SIN = (6.2831854820251465, -41.34170150756836, 81.6051025390625, -76.70254516601562,
       42.02196502685547, -14.884664535522461, 3.2164907455444336)


def horner(coefs, v):
    total = jnp.full_like(v, coefs[-1])
    for c in coefs[-2::-1]:
        total = total * v + c
    return total


def cos_sin(x, n, inv):
    r = x - jnp.floor(x * inv + 0.5) * n
    u = r * inv
    v = u * u
    return horner(COS, v), u * horner(SIN, v)


def pack_kernel(leg, out, scr):
    total = jnp.zeros((QBLK, 128), jnp.float32)
    scr[...] = total
    for s in range(SLOTS):
        out[:, MAIN * s : MAIN * (s + 1)] = leg[s, :, 0:MAIN]
        scr[:, 0:REST] = leg[s, :, MAIN:FOLD].astype(jnp.float32)
        tail = scr[...]
        total = total + (pltpu.roll(tail, REST * s, 1) if s else tail)
    out[:, SLOTS * MAIN : PACKED] = total.astype(jnp.bfloat16)


def mask_kernel(pairs, spec, out, scr):
    t_main = lax.broadcasted_iota(jnp.int32, (MAIN, 128), 0)
    t_rest = lax.broadcasted_iota(jnp.int32, (128, 128), 0) + MAIN
    for s in range(SLOTS):
        border = WAVES - pairs[s]
        border = jnp.where(pairs[s] >= 0, border, FOLD)
        main = spec[s, 0:MAIN, :].astype(jnp.float32)
        low = jnp.where(t_main < border, main, 0.0)
        out[s, 0:MAIN, 0:128] = low.astype(jnp.bfloat16)
        out[s, 0:MAIN, 128:256] = (main - low).astype(jnp.bfloat16)
        scr[...] = jnp.zeros((128, 128), jnp.float32)
        scr[REST * s : REST * (s + 1), :] = spec[s, MAIN:FOLD, :].astype(jnp.float32)
        rest = scr[...]
        low = jnp.where(t_rest - REST * s < border, rest, 0.0)
        out[s, MAIN:KP, 0:128] = low.astype(jnp.bfloat16)
        out[s, MAIN:KP, 128:256] = (rest - low).astype(jnp.bfloat16)


def legendre_kernel(place, rhs, x0, p1, m1, p2, m2, p3, m3, p4, m4, out):
    z = place[0]
    for s in range(SLOTS):
        def lhs(ref):
            return jnp.concatenate(
                [ref[:, MAIN * s : MAIN * (s + 1)], ref[:, SLOTS * MAIN : PACKED]], axis=1)
        left = jnp.concatenate([lhs(r) for r in (x0, p1, m1, p2, m2, p3, m3, p4, m4)], axis=0)
        got = jnp.dot(left, rhs[s], preferred_element_type=jnp.float32)
        for i, d in enumerate((0, 1, -1, 2, -2, 3, -3, 4)):
            block = lax.rem(z - d + 8, 8)
            for h in range(2):
                part = got[QBLK * i : QBLK * (i + 1), 128 * h : 128 * (h + 1)]
                out[pl.ds(4 * block, 4), 2 * s + h] = part.reshape(4, ROWS, 128).astype(jnp.bfloat16)


def table_kernel(lats, waves, fine, coarse):
    m = waves[...]

    def one_row(q, carry):
        a = lats[q]
        lon = 20 + 4 * jnp.minimum(a, NLAT - 1 - a)
        highest = jnp.minimum(WAVES - 1, (lon - 1) // 2).astype(jnp.float32)
        n = jnp.full((1, KP), lon, jnp.int32).astype(jnp.float32)
        inv = 1.0 / n
        scale = jnp.where((m >= 0.0) & (m <= highest), jnp.where(m == 0.0, 1.0, 2.0), 0.0)

        def at(step, count):
            j = step * lax.broadcasted_iota(jnp.int32, (count, KP), 0)
            return cos_sin(j.astype(jnp.float32) * m, n, inv)

        cos_b, sin_b = at(1, 32)
        cos_a, sin_a = at(32, 8)
        cos_a = cos_a * scale
        sin_a = sin_a * scale
        for i in range(FINE // 32):
            ca = cos_a[i : i + 1, :]
            sa = sin_a[i : i + 1, :]
            rows = slice(32 * i, 32 * (i + 1))
            fine[q, rows, 0:KP] = (ca * cos_b - sa * sin_b).astype(jnp.bfloat16)
            fine[q, rows, KP : 2 * KP] = (-(sa * cos_b + ca * sin_b)).astype(jnp.bfloat16)
        step = lax.broadcasted_iota(jnp.int32, (8, KP), 0)
        step = FINE * jnp.where(step == 0, 3, step)
        cos_c, sin_c = cos_sin(step.astype(jnp.float32) * m, n, inv)
        coarse[q, :, 0:KP] = cos_c
        coarse[q, :, KP : 2 * KP] = sin_c
        return carry

    lax.fori_loop(0, ROWS, one_row, 0)


def synth_kernel(lats, recv, tables, coarse, out, scr, turn_a, turn_b, lhs_a, lhs_b, rows,
                 fine, sems, in_sems):
    def fetch(q):
        return pltpu.make_async_copy(tables.at[q], fine.at[q], in_sems.at[q])

    for q in range(ROWS):
        fetch(q).start()
    for i in range(7):
        scr[512 * i : 512 * (i + 1), :] = (
            recv[64 * i : 64 * (i + 1)].astype(jnp.float32).reshape(512, 128))
    scr[KEEP * ROWS : KP * ROWS, :] = jnp.zeros(((KP - KEEP) * ROWS, 128), jnp.float32)

    row = lax.broadcasted_iota(jnp.int32, (128, 128), 0)
    col = lax.broadcasted_iota(jnp.int32, (128, 128), 1)
    source = jnp.where(row < 64, 2 * row, 2 * row - 127)
    perm = jnp.where(col == source, 1.0, 0.0).astype(jnp.bfloat16)
    column = lax.broadcasted_iota(jnp.int32, (64, FINE), 1)
    nt = (((1,), (1,)), ((), ()))

    def turn_row(q, turn):
        values = scr[pl.ds(q, KP, stride=ROWS), :].astype(jnp.bfloat16)
        turn[...] = lax.dot_general(perm, values, nt, preferred_element_type=jnp.float32)

    def rotate(q, turn, lhs):
        for lane in range(0, KP, 128):
            here = slice(lane, lane + 128)
            beside = slice(KP + lane, KP + lane + 128)
            for g in range(0, 64, 16):
                def put(block, left, right):
                    at = slice(64 * block + g, 64 * block + g + 16)
                    lhs[at, here] = left.astype(jnp.bfloat16)
                    lhs[at, beside] = right.astype(jnp.bfloat16)

                re = turn[g : g + 16, here]
                im = turn[64 + g : 80 + g, here]
                cc = coarse[q, 0:1, here]
                sc = coarse[q, 0:1, beside]
                re, im = cc * re - sc * im, sc * re + cc * im
                put(0, re, im)
                for step in range(1, 4):
                    cc = coarse[q, step : step + 1, here]
                    sc = coarse[q, step : step + 1, beside]
                    put(2 * step - 1, cc * re, cc * im)
                    put(2 * step, sc * im, -sc * re)

    def copy(q):
        return pltpu.make_async_copy(rows.at[q], out.at[q], sems.at[q])

    def one_row(q, lhs, other, turn, spare):
        a = lats[q]
        lon = 20 + 4 * jnp.minimum(a, NLAT - 1 - a)
        result = lax.dot_general(lhs[...], fine[q], nt, preferred_element_type=jnp.float32)
        rotate(jnp.minimum(q + 1, ROWS - 1), turn, other)
        turn_row(jnp.minimum(q + 2, ROWS - 1), spare)

        def put(jc, block):
            width = min(FINE, WIDTH - FINE * jc)
            block = jnp.where(column < lon - FINE * jc, block, 0.0).astype(jnp.bfloat16)
            rows[q, :, FINE * jc : FINE * jc + width] = block[:, 0:width]

        put(3, result[0:64, :])
        for step in range(1, 4):
            even = result[128 * step - 64 : 128 * step, :]
            odd = result[128 * step : 128 * step + 64, :]
            put(3 + step, even - odd)
            put(3 - step, even + odd)
        copy(q).start()

    def two_rows(i, carry):
        fetch(2 * i).wait()
        fetch(2 * i + 1).wait()
        one_row(2 * i, lhs_a, lhs_b, turn_b, turn_a)
        one_row(2 * i + 1, lhs_b, lhs_a, turn_a, turn_b)
        return carry

    turn_row(0, turn_a)
    turn_row(1, turn_b)
    rotate(0, turn_a, lhs_a)
    lax.fori_loop(0, ROWS // 2, two_rows, 0)
    for q in range(ROWS):
        copy(q).wait()


def cost(flops, moved):
    return pl.CostEstimate(flops=flops, transcendentals=0, bytes_accessed=moved)


def gather_pieces(x):
    def shift(v, d):
        return lax.ppermute(v, "lev", [(i, (i + d) % 8) for i in range(8)])

    p1, m1 = shift(x, 1), shift(x, -1)
    p2, m2 = shift(x, 2), shift(x, -2)
    p3, m3 = shift(p2, 1), shift(m2, -1)
    half = QBLK // 2
    p4, m4 = shift(p2[:half], 2), shift(m2[half:], -2)
    return x, p1, m1, p2, m2, p3, m3, p4, m4


def on_device(spectral, legendre, wave_pair, lat_slot):
    bf16, f32 = jnp.bfloat16, jnp.float32
    smem = pl.BlockSpec(memory_space=pltpu.SMEM)
    vmem = pl.BlockSpec(memory_space=pltpu.VMEM)
    z = lax.axis_index("lev").astype(jnp.int32)
    w = lax.axis_index("wav").astype(jnp.int32)
    own_pairs = lax.dynamic_slice_in_dim(wave_pair, w * SLOTS, SLOTS)
    own_lats = lax.dynamic_slice_in_dim(lat_slot, w * ROWS, ROWS)
    waves = jnp.stack([wave_pair, WAVES - 1 - wave_pair], axis=1)
    waves = jnp.where(wave_pair[:, None] >= 0, waves, -1).reshape(1, KEEP)
    waves = jnp.pad(waves, ((0, 0), (0, KP - KEEP)), constant_values=-1).astype(f32)

    def here(v):
        return pltpu.with_memory_space_constraint(v, pltpu.VMEM)

    def params(mib):
        return pltpu.CompilerParams(vmem_limit_bytes=mib * 2**20)

    packed = pl.pallas_call(
        pack_kernel,
        out_shape=pltpu.VMEM((QBLK, PACKED), bf16),
        in_specs=[vmem], out_specs=vmem,
        scratch_shapes=[pltpu.VMEM((QBLK, 128), f32)],
        compiler_params=params(4),
        name="pack",
    )(jnp.transpose(legendre, (0, 2, 1)))
    pieces = gather_pieces(packed)

    rhs = pl.pallas_call(
        mask_kernel,
        out_shape=pltpu.VMEM((SLOTS, KP, 256), bf16),
        in_specs=[smem, vmem], out_specs=vmem,
        scratch_shapes=[pltpu.VMEM((128, 128), f32)],
        cost_estimate=cost(2_000_000_000, 2_500_000),
        compiler_params=params(6),
        name="mask",
    )(own_pairs, spectral)

    fine, coarse = pl.pallas_call(
        table_kernel,
        out_shape=(pltpu.HBM((ROWS, FINE, 2 * KP), bf16),
                   pltpu.VMEM((ROWS, 8, 2 * KP), f32)),
        in_specs=[smem, vmem], out_specs=(vmem, vmem),
        cost_estimate=cost(4_000_000_000, 4_500_000),
        compiler_params=params(8),
        name="tables",
    )(own_lats, waves)

    fourier = pl.pallas_call(
        legendre_kernel,
        out_shape=pltpu.VMEM((32, 2 * SLOTS, ROWS, 128), bf16),
        in_specs=[smem] + [vmem] * 10, out_specs=vmem,
        cost_estimate=cost(2 * 256 * 512 * 256 * SLOTS, 4_000_000),
        compiler_params=params(12),
        name="legendre",
    )(z.reshape(1), here(rhs), *[here(p) for p in pieces])

    received = lax.all_to_all(fourier, "wav", split_axis=0, concat_axis=0, tiled=True)

    return pl.pallas_call(
        synth_kernel,
        out_shape=jax.ShapeDtypeStruct((ROWS, 64, WIDTH), bf16),
        in_specs=[smem, vmem, pl.BlockSpec(memory_space=pltpu.HBM), vmem],
        out_specs=pl.BlockSpec(memory_space=pltpu.HBM),
        scratch_shapes=[pltpu.VMEM((KP * ROWS, 128), f32),
                        pltpu.VMEM((128, KP), f32),
                        pltpu.VMEM((128, KP), f32),
                        pltpu.VMEM((64 * COARSE, 2 * KP), bf16),
                        pltpu.VMEM((64 * COARSE, 2 * KP), bf16),
                        pltpu.VMEM((ROWS, 64, WIDTH), bf16),
                        pltpu.VMEM((ROWS, FINE, 2 * KP), bf16),
                        pltpu.SemaphoreType.DMA((ROWS,)),
                        pltpu.SemaphoreType.DMA((ROWS,))],
        cost_estimate=cost(2 * 448 * 1024 * 256 * ROWS, 18_000_000),
        compiler_params=params(16),
        name="synth",
    )(own_lats, here(received.reshape(KEEP, ROWS, 128)),
      pltpu.with_memory_space_constraint(fine, pltpu.HBM), here(coarse))


def solution(mesh):
    return jax.shard_map(
        on_device,
        mesh=mesh,
        in_specs=(P("wav", None, "lev"), P("wav", None, "lev"), P(), P()),
        out_specs=P("wav", "lev", None),
        check_vma=False,
    )
```

```python
import jax
import jax.numpy as jnp
from jax import lax
from jax.experimental import pallas as pl
from jax.experimental.pallas import tpu as pltpu
from jax.sharding import PartitionSpec as P

NLAT = 800
WAVES = 400
FOLD = 401
WIDTH = 1616
SLOTS = 7
ROWS = 8
QBLK = 32
MAIN = 384
REST = FOLD - MAIN
PACKED = SLOTS * MAIN + 128
KEEP = 448
KP = 512
FINE = 256
COARSE = 7

COS = (1.0, -19.739208221435547, 64.93938446044922, -85.45662689208984, 60.24171447753906,
       -26.402057647705078, 7.7920684814453125, -1.4433850049972534)
SIN = (6.2831854820251465, -41.34170150756836, 81.6051025390625, -76.70254516601562,
       42.02196502685547, -14.884664535522461, 3.2164907455444336)


def horner(coefs, v):
    total = jnp.full_like(v, coefs[-1])
    for c in coefs[-2::-1]:
        total = total * v + c
    return total


def cos_sin(x, n, inv):
    r = x - jnp.floor(x * inv + 0.5) * n
    u = r * inv
    v = u * u
    return horner(COS, v), u * horner(SIN, v)


def pack_kernel(leg, out, scr):
    total = jnp.zeros((QBLK, 128), jnp.float32)
    scr[...] = total
    for s in range(SLOTS):
        out[:, MAIN * s : MAIN * (s + 1)] = leg[s, :, 0:MAIN]
        scr[:, 0:REST] = leg[s, :, MAIN:FOLD].astype(jnp.float32)
        tail = scr[...]
        total = total + (pltpu.roll(tail, REST * s, 1) if s else tail)
    out[:, SLOTS * MAIN : PACKED] = total.astype(jnp.bfloat16)


def mask_kernel(device, wave_pair, spec, out, scr):
    t_main = lax.broadcasted_iota(jnp.int32, (MAIN, 128), 0)
    t_rest = lax.broadcasted_iota(jnp.int32, (128, 128), 0) + MAIN
    for s in range(SLOTS):
        pair = wave_pair[device[0] * SLOTS + s]
        border = jnp.where(pair >= 0, WAVES - pair, FOLD)
        main = spec[s, 0:MAIN, :].astype(jnp.float32)
        low = jnp.where(t_main < border, main, 0.0)
        out[s, 0:MAIN, 0:128] = low.astype(jnp.bfloat16)
        out[s, 0:MAIN, 128:256] = (main - low).astype(jnp.bfloat16)
        scr[...] = jnp.zeros((128, 128), jnp.float32)
        scr[REST * s : REST * (s + 1), :] = spec[s, MAIN:FOLD, :].astype(jnp.float32)
        rest = scr[...]
        low = jnp.where(t_rest - REST * s < border, rest, 0.0)
        out[s, MAIN:KP, 0:128] = low.astype(jnp.bfloat16)
        out[s, MAIN:KP, 128:256] = (rest - low).astype(jnp.bfloat16)


def legendre_kernel(place, _tables, rhs, x0, p1, m1, p2, m2, p3, m3, p4, m4, out):
    z = place[0]
    for s in range(SLOTS):
        def lhs(ref):
            return jnp.concatenate(
                [ref[:, MAIN * s : MAIN * (s + 1)], ref[:, SLOTS * MAIN : PACKED]], axis=1)
        left = jnp.concatenate([lhs(r) for r in (x0, p1, m1, p2, m2, p3, m3, p4, m4)], axis=0)
        got = jnp.dot(left, rhs[s], preferred_element_type=jnp.float32)
        for i, d in enumerate((0, 1, -1, 2, -2, 3, -3, 4)):
            block = lax.rem(z - d + 8, 8)
            for h in range(2):
                part = got[QBLK * i : QBLK * (i + 1), 128 * h : 128 * (h + 1)]
                out[pl.ds(4 * block, 4), 2 * s + h] = part.reshape(4, ROWS, 128).astype(jnp.bfloat16)


def table_kernel(device, lat_slot, pairs, fine_out, coarse_out, scr, fine, coarse, sems):
    def copies(q):
        return (pltpu.make_async_copy(fine.at[q], fine_out.at[q], sems.at[0, q]),
                pltpu.make_async_copy(coarse.at[q], coarse_out.at[q], sems.at[1, q]))

    scr[...] = jnp.full((1, KP), -1, jnp.int32)
    scr[:, 0:KEEP] = pairs[...]
    pair = scr[...]
    half = lax.broadcasted_iota(jnp.int32, (1, KP), 1) % 2
    m = jnp.where(pair < 0, -1, jnp.where(half == 0, pair, WAVES - 1 - pair)).astype(jnp.float32)

    def one_row(q, carry):
        a = lat_slot[device[0] * ROWS + q]
        lon = 20 + 4 * jnp.minimum(a, NLAT - 1 - a)
        highest = jnp.minimum(WAVES - 1, (lon - 1) // 2).astype(jnp.float32)
        n = jnp.full((1, KP), lon, jnp.int32).astype(jnp.float32)
        inv = 1.0 / n
        scale = jnp.where((m >= 0.0) & (m <= highest), jnp.where(m == 0.0, 1.0, 2.0), 0.0)

        def at(step, count):
            j = step * lax.broadcasted_iota(jnp.int32, (count, KP), 0)
            return cos_sin(j.astype(jnp.float32) * m, n, inv)

        cos_b, sin_b = at(1, 32)
        cos_a, sin_a = at(32, 8)
        cos_a = cos_a * scale
        sin_a = sin_a * scale
        for i in range(FINE // 32):
            ca = cos_a[i : i + 1, :]
            sa = sin_a[i : i + 1, :]
            rows = slice(32 * i, 32 * (i + 1))
            fine[q, rows, 0:KP] = (ca * cos_b - sa * sin_b).astype(jnp.bfloat16)
            fine[q, rows, KP : 2 * KP] = (-(sa * cos_b + ca * sin_b)).astype(jnp.bfloat16)
        step = lax.broadcasted_iota(jnp.int32, (8, KP), 0)
        step = FINE * jnp.where(step == 0, 3, step)
        cos_c, sin_c = cos_sin(step.astype(jnp.float32) * m, n, inv)
        coarse[q, :, 0:KP] = cos_c
        coarse[q, :, KP : 2 * KP] = sin_c
        for copy in copies(q):
            copy.start()
        return carry

    lax.fori_loop(0, ROWS, one_row, 0)
    for q in range(ROWS):
        for copy in copies(q):
            copy.wait()


def synth_kernel(device, lat_slot, recv, fine, coarse, out, scr, turn_a, turn_b, lhs_a, lhs_b, rows, sems):
    for i in range(7):
        scr[512 * i : 512 * (i + 1), :] = (
            recv[64 * i : 64 * (i + 1)].astype(jnp.float32).reshape(512, 128))
    scr[KEEP * ROWS : KP * ROWS, :] = jnp.zeros(((KP - KEEP) * ROWS, 128), jnp.float32)

    row = lax.broadcasted_iota(jnp.int32, (128, 128), 0)
    col = lax.broadcasted_iota(jnp.int32, (128, 128), 1)
    source = jnp.where(row < 64, 2 * row, 2 * row - 127)
    perm = jnp.where(col == source, 1.0, 0.0).astype(jnp.bfloat16)
    column = lax.broadcasted_iota(jnp.int32, (64, FINE), 1)
    nt = (((1,), (1,)), ((), ()))

    def turn_row(q, turn):
        values = scr[pl.ds(q, KP, stride=ROWS), :].astype(jnp.bfloat16)
        turn[...] = lax.dot_general(perm, values, nt, preferred_element_type=jnp.float32)

    def rotate(q, turn, lhs):
        for lane in range(0, KP, 128):
            here = slice(lane, lane + 128)
            beside = slice(KP + lane, KP + lane + 128)
            for g in range(0, 64, 16):
                def put(block, left, right):
                    at = slice(64 * block + g, 64 * block + g + 16)
                    lhs[at, here] = left.astype(jnp.bfloat16)
                    lhs[at, beside] = right.astype(jnp.bfloat16)

                re = turn[g : g + 16, here]
                im = turn[64 + g : 80 + g, here]
                cc = coarse[q, 0:1, here]
                sc = coarse[q, 0:1, beside]
                re, im = cc * re - sc * im, sc * re + cc * im
                put(0, re, im)
                for step in range(1, 4):
                    cc = coarse[q, step : step + 1, here]
                    sc = coarse[q, step : step + 1, beside]
                    put(2 * step - 1, cc * re, cc * im)
                    put(2 * step, sc * im, -sc * re)

    def copy(q):
        return pltpu.make_async_copy(rows.at[q], out.at[q], sems.at[q])

    def one_row(q, lhs, other, turn, spare):
        a = lat_slot[device[0] * ROWS + q]
        lon = 20 + 4 * jnp.minimum(a, NLAT - 1 - a)
        result = lax.dot_general(lhs[...], fine[q], nt, preferred_element_type=jnp.float32)
        rotate(jnp.minimum(q + 1, ROWS - 1), turn, other)
        turn_row(jnp.minimum(q + 2, ROWS - 1), spare)

        def put(jc, block):
            width = min(FINE, WIDTH - FINE * jc)
            block = jnp.where(column < lon - FINE * jc, block, 0.0).astype(jnp.bfloat16)
            rows[q, :, FINE * jc : FINE * jc + width] = block[:, 0:width]

        put(3, result[0:64, :])
        for step in range(1, 4):
            even = result[128 * step - 64 : 128 * step, :]
            odd = result[128 * step : 128 * step + 64, :]
            put(3 + step, even - odd)
            put(3 - step, even + odd)
        copy(q).start()

    def two_rows(i, carry):
        one_row(2 * i, lhs_a, lhs_b, turn_b, turn_a)
        one_row(2 * i + 1, lhs_b, lhs_a, turn_a, turn_b)
        return carry

    turn_row(0, turn_a)
    turn_row(1, turn_b)
    rotate(0, turn_a, lhs_a)
    lax.fori_loop(0, ROWS // 2, two_rows, 0)
    for q in range(ROWS):
        copy(q).wait()


def cost(flops, moved):
    return pl.CostEstimate(flops=flops, transcendentals=0, bytes_accessed=moved)


def half_of(x, first):
    def kernel(ref, out):
        out[...] = ref[first : first + QBLK // 2, :]

    return pl.pallas_call(
        kernel,
        out_shape=pltpu.VMEM((QBLK // 2, PACKED), jnp.bfloat16),
        in_specs=[pl.BlockSpec(memory_space=pltpu.VMEM)],
        out_specs=pl.BlockSpec(memory_space=pltpu.VMEM),
        compiler_params=pltpu.CompilerParams(vmem_limit_bytes=2**21),
        name="half",
    )(pltpu.with_memory_space_constraint(x, pltpu.VMEM))


def gather_pieces(x):
    def shift(v, d):
        return lax.ppermute(v, "lev", [(i, (i + d) % 8) for i in range(8)])

    p1, m1 = shift(x, 1), shift(x, -1)
    p2, m2 = shift(x, 2), shift(x, -2)
    p3, m3 = shift(p2, 1), shift(m2, -1)
    p4, m4 = shift(half_of(p2, 0), 2), shift(half_of(m2, QBLK // 2), -2)
    return x, p1, m1, p2, m2, p3, m3, p4, m4


def on_device(spectral, legendre, wave_pair, lat_slot):
    bf16, f32 = jnp.bfloat16, jnp.float32
    smem = pl.BlockSpec(memory_space=pltpu.SMEM)
    vmem = pl.BlockSpec(memory_space=pltpu.VMEM)
    hbm = pl.BlockSpec(memory_space=pltpu.HBM)
    z = lax.axis_index("lev").astype(jnp.int32)
    w = lax.axis_index("wav").astype(jnp.int32)
    device = w.reshape(1)
    pairs = jnp.broadcast_to(wave_pair[:, None], (KEEP // 2, 2)).reshape(1, KEEP)

    def here(v):
        return pltpu.with_memory_space_constraint(v, pltpu.VMEM)

    def params(mib):
        return pltpu.CompilerParams(vmem_limit_bytes=mib * 2**20)

    packed = pl.pallas_call(
        pack_kernel,
        out_shape=pltpu.VMEM((QBLK, PACKED), bf16),
        in_specs=[vmem], out_specs=vmem,
        scratch_shapes=[pltpu.VMEM((QBLK, 128), f32)],
        compiler_params=params(4),
        name="pack",
    )(jnp.transpose(legendre, (0, 2, 1)))
    pieces = gather_pieces(packed)

    rhs = pl.pallas_call(
        mask_kernel,
        out_shape=pltpu.VMEM((SLOTS, KP, 256), bf16),
        in_specs=[smem, smem, vmem], out_specs=vmem,
        scratch_shapes=[pltpu.VMEM((128, 128), f32)],
        cost_estimate=cost(2_000_000_000, 2_500_000),
        compiler_params=params(6),
        name="mask",
    )(device, wave_pair, spectral)

    fine, coarse = pl.pallas_call(
        table_kernel,
        out_shape=(pltpu.HBM((ROWS, FINE, 2 * KP), bf16),
                   pltpu.HBM((ROWS, 8, 2 * KP), f32)),
        in_specs=[smem, smem, vmem], out_specs=(hbm, hbm),
        scratch_shapes=[pltpu.VMEM((1, KP), jnp.int32),
                        pltpu.VMEM((ROWS, FINE, 2 * KP), bf16),
                        pltpu.VMEM((ROWS, 8, 2 * KP), f32),
                        pltpu.SemaphoreType.DMA((2, ROWS))],
        cost_estimate=cost(4_000_000_000, 4_500_000),
        compiler_params=params(8),
        name="tables",
    )(device, lat_slot, pairs)

    fourier = pl.pallas_call(
        legendre_kernel,
        out_shape=pltpu.VMEM((32, 2 * SLOTS, ROWS, 128), bf16),
        in_specs=[smem, hbm] + [vmem] * 10, out_specs=vmem,
        cost_estimate=cost(2 * 256 * 512 * 256 * SLOTS, 4_000_000),
        compiler_params=params(12),
        name="legendre",
    )(z.reshape(1), pltpu.with_memory_space_constraint(coarse, pltpu.HBM), here(rhs), *[here(p) for p in pieces])

    received = lax.all_to_all(fourier, "wav", split_axis=0, concat_axis=0, tiled=True)

    return pl.pallas_call(
        synth_kernel,
        out_shape=jax.ShapeDtypeStruct((ROWS, 64, WIDTH), bf16),
        in_specs=[smem, smem, vmem, vmem, vmem],
        out_specs=pl.BlockSpec(memory_space=pltpu.HBM),
        scratch_shapes=[pltpu.VMEM((KP * ROWS, 128), f32),
                        pltpu.VMEM((128, KP), f32),
                        pltpu.VMEM((128, KP), f32),
                        pltpu.VMEM((64 * COARSE, 2 * KP), bf16),
                        pltpu.VMEM((64 * COARSE, 2 * KP), bf16),
                        pltpu.VMEM((ROWS, 64, WIDTH), bf16),
                        pltpu.SemaphoreType.DMA((ROWS,))],
        cost_estimate=cost(2 * 448 * 1024 * 256 * ROWS, 18_000_000),
        compiler_params=params(16),
        name="synth",
    )(device, lat_slot, here(received.reshape(KEEP, ROWS, 128)),
      here(fine), here(coarse))


def solution(mesh):
    return jax.shard_map(
        on_device,
        mesh=mesh,
        in_specs=(P("wav", None, "lev"), P("wav", None, "lev"), P(), P()),
        out_specs=P("wav", "lev", None),
        check_vma=False,
    )
```

```python
import jax
import jax.numpy as jnp
from jax import lax
from jax.experimental import pallas as pl
from jax.experimental.pallas import tpu as pltpu
from jax.sharding import PartitionSpec as P


NLAT = 800
WAVES = 400
FOLD = 401
WIDTH = 1616
SLOTS = 7
ROWS = 8
QBLK = 32
MAIN = 384
REST = FOLD - MAIN
PACKED = SLOTS * MAIN + 128
KEEP = 448
KP = 512
FINE = 256
COARSE = 7

COS = (1.0, -19.739208221435547, 64.93938446044922, -85.45662689208984, 60.24171447753906,
       -26.402057647705078, 7.7920684814453125, -1.4433850049972534)
SIN = (6.2831854820251465, -41.34170150756836, 81.6051025390625, -76.70254516601562,
       42.02196502685547, -14.884664535522461, 3.2164907455444336)


def horner(coefs, v):
    total = jnp.full_like(v, coefs[-1])
    for c in coefs[-2::-1]:
        total = total * v + c
    return total


def cos_sin(x, n, inv):
    r = x - jnp.floor(x * inv + 0.5) * n
    u = r * inv
    v = u * u
    return horner(COS, v), u * horner(SIN, v)


def pack_kernel(leg, out, scr):
    total = jnp.zeros((QBLK, 128), jnp.float32)
    scr[...] = total
    for s in range(SLOTS):
        out[:, MAIN * s : MAIN * (s + 1)] = leg[s, :, 0:MAIN]
        scr[:, 0:REST] = leg[s, :, MAIN:FOLD].astype(jnp.float32)
        tail = scr[...]
        total = total + (pltpu.roll(tail, REST * s, 1) if s else tail)
    out[:, SLOTS * MAIN : PACKED] = total.astype(jnp.bfloat16)


def mask_kernel(device, wave_pair, spec, out, scr):
    t_main = lax.broadcasted_iota(jnp.int32, (MAIN, 128), 0)
    t_rest = lax.broadcasted_iota(jnp.int32, (128, 128), 0) + MAIN
    for s in range(SLOTS):
        pair = wave_pair[device[0] * SLOTS + s]
        border = jnp.where(pair >= 0, WAVES - pair, FOLD)
        main = spec[s, 0:MAIN, :].astype(jnp.float32)
        low = jnp.where(t_main < border, main, 0.0)
        out[s, 0:MAIN, 0:128] = low.astype(jnp.bfloat16)
        out[s, 0:MAIN, 128:256] = (main - low).astype(jnp.bfloat16)
        scr[...] = jnp.zeros((128, 128), jnp.float32)
        scr[REST * s : REST * (s + 1), :] = spec[s, MAIN:FOLD, :].astype(jnp.float32)
        rest = scr[...]
        low = jnp.where(t_rest - REST * s < border, rest, 0.0)
        out[s, MAIN:KP, 0:128] = low.astype(jnp.bfloat16)
        out[s, MAIN:KP, 128:256] = (rest - low).astype(jnp.bfloat16)


def legendre_blocks(place, rhs, refs, offsets, out):
    z = place[0]
    for s in range(SLOTS):
        def lhs(ref):
            return jnp.concatenate(
                [ref[:, MAIN * s : MAIN * (s + 1)], ref[:, SLOTS * MAIN : PACKED]], axis=1)

        left = jnp.concatenate([lhs(r) for r in refs], axis=0)
        got = jnp.dot(left, rhs[s], preferred_element_type=jnp.float32)
        for i, d in enumerate(offsets):
            block = lax.rem(z - d + 8, 8)
            for h in range(2):
                part = got[QBLK * i : QBLK * (i + 1), 128 * h : 128 * (h + 1)]
                out[pl.ds(4 * block, 4), 2 * s + h] = part.reshape(4, ROWS, 128).astype(jnp.bfloat16)


def near_kernel(place, rhs, x0, p1, m1, p2, m2, out):
    legendre_blocks(place, rhs, (x0, p1, m1, p2, m2), (0, 1, -1, 2, -2), out)


def far_kernel(place, _tables, _near, rhs, p3, m3, p4, m4, out):
    legendre_blocks(place, rhs, (p3, m3, p4, m4), (3, -3, 4), out)


def table_kernel(device, lat_slot, pairs, fine_out, coarse_out, scr, fine, coarse, sems):
    def copies(q):
        return (pltpu.make_async_copy(fine.at[q], fine_out.at[q], sems.at[0, q]),
                pltpu.make_async_copy(coarse.at[q], coarse_out.at[q], sems.at[1, q]))

    scr[...] = jnp.full((1, KP), -1, jnp.int32)
    scr[:, 0:KEEP] = pairs[...]
    pair = scr[...]
    half = lax.broadcasted_iota(jnp.int32, (1, KP), 1) % 2
    m = jnp.where(pair < 0, -1, jnp.where(half == 0, pair, WAVES - 1 - pair)).astype(jnp.float32)

    def one_row(q, carry):
        a = lat_slot[device[0] * ROWS + q]
        lon = 20 + 4 * jnp.minimum(a, NLAT - 1 - a)
        highest = jnp.minimum(WAVES - 1, (lon - 1) // 2).astype(jnp.float32)
        n = jnp.full((1, KP), lon, jnp.int32).astype(jnp.float32)
        inv = 1.0 / n
        scale = jnp.where((m >= 0.0) & (m <= highest), jnp.where(m == 0.0, 1.0, 2.0), 0.0)

        def at(step, count):
            j = step * lax.broadcasted_iota(jnp.int32, (count, KP), 0)
            return cos_sin(j.astype(jnp.float32) * m, n, inv)

        cos_b, sin_b = at(1, 32)
        cos_a, sin_a = at(32, 8)
        cos_a = cos_a * scale
        sin_a = sin_a * scale
        for i in range(FINE // 32):
            ca = cos_a[i : i + 1, :]
            sa = sin_a[i : i + 1, :]
            rows = slice(32 * i, 32 * (i + 1))
            fine[q, rows, 0:KP] = (ca * cos_b - sa * sin_b).astype(jnp.bfloat16)
            fine[q, rows, KP : 2 * KP] = (-(sa * cos_b + ca * sin_b)).astype(jnp.bfloat16)
        step = lax.broadcasted_iota(jnp.int32, (8, KP), 0)
        step = FINE * jnp.where(step == 0, 3, step)
        cos_c, sin_c = cos_sin(step.astype(jnp.float32) * m, n, inv)
        coarse[q, :, 0:KP] = cos_c
        coarse[q, :, KP : 2 * KP] = sin_c
        for copy in copies(q):
            copy.start()
        return carry

    lax.fori_loop(0, ROWS, one_row, 0)
    for q in range(ROWS):
        for copy in copies(q):
            copy.wait()


def synth_kernel(device, lat_slot, recv, fine, coarse, out, scr, turn_a, turn_b, lhs_a, lhs_b, rows, sems):
    for i in range(7):
        scr[512 * i : 512 * (i + 1), :] = (
            recv[64 * i : 64 * (i + 1)].astype(jnp.float32).reshape(512, 128))
    scr[KEEP * ROWS : KP * ROWS, :] = jnp.zeros(((KP - KEEP) * ROWS, 128), jnp.float32)

    row = lax.broadcasted_iota(jnp.int32, (128, 128), 0)
    col = lax.broadcasted_iota(jnp.int32, (128, 128), 1)
    source = jnp.where(row < 64, 2 * row, 2 * row - 127)
    perm = jnp.where(col == source, 1.0, 0.0).astype(jnp.bfloat16)
    column = lax.broadcasted_iota(jnp.int32, (64, FINE), 1)
    nt = (((1,), (1,)), ((), ()))

    def turn_row(q, turn):
        values = scr[pl.ds(q, KP, stride=ROWS), :].astype(jnp.bfloat16)
        turn[...] = lax.dot_general(perm, values, nt, preferred_element_type=jnp.float32)

    def rotate(q, turn, lhs):
        for lane in range(0, KP, 128):
            here = slice(lane, lane + 128)
            beside = slice(KP + lane, KP + lane + 128)
            for g in range(0, 64, 16):
                def put(block, left, right):
                    at = slice(64 * block + g, 64 * block + g + 16)
                    lhs[at, here] = left.astype(jnp.bfloat16)
                    lhs[at, beside] = right.astype(jnp.bfloat16)

                re = turn[g : g + 16, here]
                im = turn[64 + g : 80 + g, here]
                cc = coarse[q, 0:1, here]
                sc = coarse[q, 0:1, beside]
                re, im = cc * re - sc * im, sc * re + cc * im
                put(0, re, im)
                for step in range(1, 4):
                    cc = coarse[q, step : step + 1, here]
                    sc = coarse[q, step : step + 1, beside]
                    put(2 * step - 1, cc * re, cc * im)
                    put(2 * step, sc * im, -sc * re)

    def copy(q):
        return pltpu.make_async_copy(rows.at[q], out.at[q], sems.at[q])

    def one_row(q, lhs, other, turn, spare):
        a = lat_slot[device[0] * ROWS + q]
        lon = 20 + 4 * jnp.minimum(a, NLAT - 1 - a)
        result = lax.dot_general(lhs[...], fine[q], nt, preferred_element_type=jnp.float32)
        if other is not None:
            rotate(q + 1, turn, other)
        if spare is not None:
            turn_row(q + 2, spare)

        def put(jc, block):
            width = min(FINE, WIDTH - FINE * jc)
            block = jnp.where(column < lon - FINE * jc, block, 0.0).astype(jnp.bfloat16)
            rows[q, :, FINE * jc : FINE * jc + width] = block[:, 0:width]

        put(3, result[0:64, :])
        for step in range(1, 4):
            even = result[128 * step - 64 : 128 * step, :]
            odd = result[128 * step : 128 * step + 64, :]
            put(3 + step, even - odd)
            put(3 - step, even + odd)
        copy(q).start()

    def two_rows(i, carry):
        one_row(2 * i, lhs_a, lhs_b, turn_b, turn_a)
        one_row(2 * i + 1, lhs_b, lhs_a, turn_a, turn_b)
        return carry

    turn_row(0, turn_a)
    turn_row(1, turn_b)
    rotate(0, turn_a, lhs_a)
    lax.fori_loop(0, ROWS // 2 - 1, two_rows, 0)
    one_row(ROWS - 2, lhs_a, lhs_b, turn_b, None)
    one_row(ROWS - 1, lhs_b, None, None, None)
    for q in range(ROWS):
        copy(q).wait()


def cost(flops, moved):
    return pl.CostEstimate(flops=flops, transcendentals=0, bytes_accessed=moved)


def half_of(x, first):
    def kernel(ref, out):
        out[...] = ref[first : first + QBLK // 2, :]

    return pl.pallas_call(
        kernel,
        out_shape=pltpu.VMEM((QBLK // 2, PACKED), jnp.bfloat16),
        in_specs=[pl.BlockSpec(memory_space=pltpu.VMEM)],
        out_specs=pl.BlockSpec(memory_space=pltpu.VMEM),
        compiler_params=pltpu.CompilerParams(vmem_limit_bytes=2**21),
        name="half",
    )(pltpu.with_memory_space_constraint(x, pltpu.VMEM))


def gather_pieces(x):
    def shift(v, d):
        return lax.ppermute(v, "lev", [(i, (i + d) % 8) for i in range(8)])

    p1, m1 = shift(x, 1), shift(x, -1)
    p2, m2 = shift(x, 2), shift(x, -2)
    p3, m3 = shift(p2, 1), shift(m2, -1)
    p4, m4 = shift(half_of(p2, 0), 2), shift(half_of(m2, QBLK // 2), -2)
    return x, p1, m1, p2, m2, p3, m3, p4, m4


def program(spectral, legendre, wave_pair, lat_slot):
    bf16, f32 = jnp.bfloat16, jnp.float32
    smem = pl.BlockSpec(memory_space=pltpu.SMEM)
    vmem = pl.BlockSpec(memory_space=pltpu.VMEM)
    hbm = pl.BlockSpec(memory_space=pltpu.HBM)
    z = lax.axis_index("lev").astype(jnp.int32)
    w = lax.axis_index("wav").astype(jnp.int32)
    device = w.reshape(1)
    pairs = jnp.broadcast_to(wave_pair[:, None], (KEEP // 2, 2)).reshape(1, KEEP)

    def here(v):
        return pltpu.with_memory_space_constraint(v, pltpu.VMEM)

    def params(mib):
        return pltpu.CompilerParams(vmem_limit_bytes=mib * 2**20)

    packed = pl.pallas_call(
        pack_kernel,
        out_shape=pltpu.VMEM((QBLK, PACKED), bf16),
        in_specs=[vmem], out_specs=vmem,
        scratch_shapes=[pltpu.VMEM((QBLK, 128), f32)],
        compiler_params=params(4),
        name="pack",
    )(jnp.transpose(legendre, (0, 2, 1)))
    pieces = gather_pieces(packed)

    rhs = pl.pallas_call(
        mask_kernel,
        out_shape=pltpu.VMEM((SLOTS, KP, 256), bf16),
        in_specs=[smem, smem, vmem], out_specs=vmem,
        scratch_shapes=[pltpu.VMEM((128, 128), f32)],
        cost_estimate=cost(2_000_000_000, 2_500_000),
        compiler_params=params(6),
        name="mask",
    )(device, wave_pair, spectral)

    fine, coarse = pl.pallas_call(
        table_kernel,
        out_shape=(pltpu.HBM((ROWS, FINE, 2 * KP), bf16),
                   pltpu.HBM((ROWS, 8, 2 * KP), f32)),
        in_specs=[smem, smem, vmem], out_specs=(hbm, hbm),
        scratch_shapes=[pltpu.VMEM((1, KP), jnp.int32),
                        pltpu.VMEM((ROWS, FINE, 2 * KP), bf16),
                        pltpu.VMEM((ROWS, 8, 2 * KP), f32),
                        pltpu.SemaphoreType.DMA((2, ROWS))],
        cost_estimate=cost(4_000_000_000, 4_500_000),
        compiler_params=params(8),
        name="tables",
    )(device, lat_slot, pairs)

    near = pl.pallas_call(
        near_kernel,
        out_shape=pltpu.VMEM((32, 2 * SLOTS, ROWS, 128), bf16),
        in_specs=[smem] + [vmem] * 6, out_specs=vmem,
        cost_estimate=cost(1_000_000_000, 3_000_000),
        compiler_params=params(8),
        name="near",
    )(z.reshape(1), here(rhs), *[here(p) for p in pieces[:5]])

    fourier = pl.pallas_call(
        far_kernel,
        out_shape=pltpu.VMEM((32, 2 * SLOTS, ROWS, 128), bf16),
        in_specs=[smem, hbm] + [vmem] * 6, out_specs=vmem,
        input_output_aliases={2: 0},
        cost_estimate=cost(2 * 96 * 512 * 256 * SLOTS, 2_000_000),
        compiler_params=params(8),
        name="far",
    )(z.reshape(1), pltpu.with_memory_space_constraint(coarse, pltpu.HBM), here(near), here(rhs),
      *[here(p) for p in pieces[5:]])

    received = lax.all_to_all(fourier, "wav", split_axis=0, concat_axis=0, tiled=True)

    return pl.pallas_call(
        synth_kernel,
        out_shape=jax.ShapeDtypeStruct((ROWS, 64, WIDTH), bf16),
        in_specs=[smem, smem, vmem, vmem, vmem],
        out_specs=pl.BlockSpec(memory_space=pltpu.HBM),
        scratch_shapes=[pltpu.VMEM((KP * ROWS, 128), f32),
                        pltpu.VMEM((128, KP), f32),
                        pltpu.VMEM((128, KP), f32),
                        pltpu.VMEM((64 * COARSE, 2 * KP), bf16),
                        pltpu.VMEM((64 * COARSE, 2 * KP), bf16),
                        pltpu.VMEM((ROWS, 64, WIDTH), bf16),
                        pltpu.SemaphoreType.DMA((ROWS,))],
        cost_estimate=cost(2 * 448 * 1024 * 256 * ROWS, 18_000_000),
        compiler_params=params(16),
        name="synth",
    )(device, lat_slot, here(received.reshape(KEEP, ROWS, 128)),
      here(fine), here(coarse))


def solution(mesh):
    return jax.shard_map(
        program,
        mesh=mesh,
        in_specs=(P("wav", None, "lev"), P("wav", None, "lev"), P(), P()),
        out_specs=P("wav", "lev", None),
        check_vma=False,
    )
```

```python
import jax
import jax.numpy as jnp
from jax import lax
from jax.experimental import pallas as pl
from jax.experimental.pallas import tpu as pltpu
from jax.sharding import PartitionSpec as P


NLAT = 800
WAVES = 400
FOLD = 401
WIDTH = 1616
SLOTS = 7
ROWS = 8
QBLK = 32
MAIN = 384
REST = FOLD - MAIN
PACKED = SLOTS * MAIN + 128
KEEP = 448
KP = 512
FINE = 256
COARSE = 7

COS = (1.0, -19.739208221435547, 64.93938446044922, -85.45662689208984, 60.24171447753906,
       -26.402057647705078, 7.7920684814453125, -1.4433850049972534)
SIN = (6.2831854820251465, -41.34170150756836, 81.6051025390625, -76.70254516601562,
       42.02196502685547, -14.884664535522461, 3.2164907455444336)


def horner(coefs, v):
    total = jnp.full_like(v, coefs[-1])
    for c in coefs[-2::-1]:
        total = total * v + c
    return total


def cos_sin(x, n, inv):
    r = x - jnp.floor(x * inv + 0.5) * n
    u = r * inv
    v = u * u
    return horner(COS, v), u * horner(SIN, v)


def pack_kernel(source, out, scr, leg, sems):
    def fetch(s):
        return pltpu.make_async_copy(source.at[s], leg.at[s], sems.at[s])

    for s in range(SLOTS):
        fetch(s).start()
    total = jnp.zeros((QBLK, 128), jnp.float32)
    scr[...] = total
    for s in range(SLOTS):
        fetch(s).wait()
        out[:, MAIN * s : MAIN * (s + 1)] = leg[s, :, 0:MAIN]
        scr[:, 0:REST] = leg[s, :, MAIN:FOLD].astype(jnp.float32)
        tail = scr[...]
        total = total + (pltpu.roll(tail, REST * s, 1) if s else tail)
    out[:, SLOTS * MAIN : PACKED] = total.astype(jnp.bfloat16)


def mask_kernel(device, wave_pair, spec, out, scr):
    t_main = lax.broadcasted_iota(jnp.int32, (MAIN, 128), 0)
    t_rest = lax.broadcasted_iota(jnp.int32, (128, 128), 0) + MAIN
    for s in range(SLOTS):
        pair = wave_pair[device[0] * SLOTS + s]
        border = jnp.where(pair >= 0, WAVES - pair, FOLD)
        main = spec[s, 0:MAIN, :].astype(jnp.float32)
        low = jnp.where(t_main < border, main, 0.0)
        out[s, 0:MAIN, 0:128] = low.astype(jnp.bfloat16)
        out[s, 0:MAIN, 128:256] = (main - low).astype(jnp.bfloat16)
        scr[...] = jnp.zeros((128, 128), jnp.float32)
        scr[REST * s : REST * (s + 1), :] = spec[s, MAIN:FOLD, :].astype(jnp.float32)
        rest = scr[...]
        low = jnp.where(t_rest - REST * s < border, rest, 0.0)
        out[s, MAIN:KP, 0:128] = low.astype(jnp.bfloat16)
        out[s, MAIN:KP, 128:256] = (rest - low).astype(jnp.bfloat16)


def legendre_blocks(place, rhs, refs, offsets, out):
    z = place[0]
    for s in range(SLOTS):
        def lhs(ref):
            return jnp.concatenate(
                [ref[:, MAIN * s : MAIN * (s + 1)], ref[:, SLOTS * MAIN : PACKED]], axis=1)

        left = jnp.concatenate([lhs(r) for r in refs], axis=0)
        got = jnp.dot(left, rhs[s], preferred_element_type=jnp.float32)
        for i, d in enumerate(offsets):
            block = lax.rem(z - d + 8, 8)
            for h in range(2):
                part = got[QBLK * i : QBLK * (i + 1), 128 * h : 128 * (h + 1)]
                out[pl.ds(4 * block, 4), 2 * s + h] = part.reshape(4, ROWS, 128).astype(jnp.bfloat16)


def near_kernel(place, rhs, x0, p1, m1, p2, m2, out):
    legendre_blocks(place, rhs, (x0, p1, m1, p2, m2), (0, 1, -1, 2, -2), out)


def far_kernel(place, _tables, _near, rhs, p3, m3, p4, m4, out):
    legendre_blocks(place, rhs, (p3, m3, p4, m4), (3, -3, 4), out)


def table_kernel(device, lat_slot, pairs, fine_out, coarse_out, scr, fine, coarse, sems):
    def copies(q):
        return (pltpu.make_async_copy(fine.at[q], fine_out.at[q], sems.at[0, q]),
                pltpu.make_async_copy(coarse.at[q], coarse_out.at[q], sems.at[1, q]))

    scr[...] = jnp.full((1, KP), -1, jnp.int32)
    scr[:, 0:KEEP] = pairs[...]
    pair = scr[...]
    half = lax.broadcasted_iota(jnp.int32, (1, KP), 1) % 2
    m = jnp.where(pair < 0, -1, jnp.where(half == 0, pair, WAVES - 1 - pair)).astype(jnp.float32)

    def one_row(q, carry):
        a = lat_slot[device[0] * ROWS + q]
        lon = 20 + 4 * jnp.minimum(a, NLAT - 1 - a)
        highest = jnp.minimum(WAVES - 1, (lon - 1) // 2).astype(jnp.float32)
        n = jnp.full((1, KP), lon, jnp.int32).astype(jnp.float32)
        inv = 1.0 / n
        scale = jnp.where((m >= 0.0) & (m <= highest), jnp.where(m == 0.0, 1.0, 2.0), 0.0)

        def at(step, count):
            j = step * lax.broadcasted_iota(jnp.int32, (count, KP), 0)
            return cos_sin(j.astype(jnp.float32) * m, n, inv)

        cos_b, sin_b = at(1, 32)
        cos_a, sin_a = at(32, 8)
        cos_a = cos_a * scale
        sin_a = sin_a * scale
        for i in range(FINE // 32):
            ca = cos_a[i : i + 1, :]
            sa = sin_a[i : i + 1, :]
            rows = slice(32 * i, 32 * (i + 1))
            fine[q, rows, 0:KP] = (ca * cos_b - sa * sin_b).astype(jnp.bfloat16)
            fine[q, rows, KP : 2 * KP] = (-(sa * cos_b + ca * sin_b)).astype(jnp.bfloat16)
        step = lax.broadcasted_iota(jnp.int32, (8, KP), 0)
        step = FINE * jnp.where(step == 0, 3, step)
        cos_c, sin_c = cos_sin(step.astype(jnp.float32) * m, n, inv)
        coarse[q, :, 0:KP] = cos_c
        coarse[q, :, KP : 2 * KP] = sin_c
        for copy in copies(q):
            copy.start()
        return carry

    lax.fori_loop(0, ROWS, one_row, 0)
    for q in range(ROWS):
        for copy in copies(q):
            copy.wait()


def synth_kernel(device, lat_slot, recv, fine, coarse, out, scr, turn_a, turn_b, lhs_a, lhs_b, rows, sems):
    for i in range(7):
        scr[512 * i : 512 * (i + 1), :] = (
            recv[64 * i : 64 * (i + 1)].astype(jnp.float32).reshape(512, 128))
    scr[KEEP * ROWS : KP * ROWS, :] = jnp.zeros(((KP - KEEP) * ROWS, 128), jnp.float32)

    row = lax.broadcasted_iota(jnp.int32, (128, 128), 0)
    col = lax.broadcasted_iota(jnp.int32, (128, 128), 1)
    source = jnp.where(row < 64, 2 * row, 2 * row - 127)
    perm = jnp.where(col == source, 1.0, 0.0).astype(jnp.bfloat16)
    column = lax.broadcasted_iota(jnp.int32, (64, FINE), 1)
    nt = (((1,), (1,)), ((), ()))

    def turn_row(q, turn):
        values = scr[pl.ds(q, KP, stride=ROWS), :].astype(jnp.bfloat16)
        turn[...] = lax.dot_general(perm, values, nt, preferred_element_type=jnp.float32)

    def rotate(q, turn, lhs):
        for lane in range(0, KP, 128):
            here = slice(lane, lane + 128)
            beside = slice(KP + lane, KP + lane + 128)
            for g in range(0, 64, 16):
                def put(block, left, right):
                    at = slice(64 * block + g, 64 * block + g + 16)
                    lhs[at, here] = left.astype(jnp.bfloat16)
                    lhs[at, beside] = right.astype(jnp.bfloat16)

                re = turn[g : g + 16, here]
                im = turn[64 + g : 80 + g, here]
                cc = coarse[q, 0:1, here]
                sc = coarse[q, 0:1, beside]
                re, im = cc * re - sc * im, sc * re + cc * im
                put(0, re, im)
                for step in range(1, 4):
                    cc = coarse[q, step : step + 1, here]
                    sc = coarse[q, step : step + 1, beside]
                    put(2 * step - 1, cc * re, cc * im)
                    put(2 * step, sc * im, -sc * re)

    def copy(q):
        return pltpu.make_async_copy(rows.at[q], out.at[q], sems.at[q])

    def one_row(q, lhs, other, turn, spare):
        a = lat_slot[device[0] * ROWS + q]
        lon = 20 + 4 * jnp.minimum(a, NLAT - 1 - a)
        result = lax.dot_general(lhs[...], fine[q], nt, preferred_element_type=jnp.float32)
        if other is not None:
            rotate(q + 1, turn, other)
        if spare is not None:
            turn_row(q + 2, spare)

        def put(jc, block):
            width = min(FINE, WIDTH - FINE * jc)
            block = jnp.where(column < lon - FINE * jc, block, 0.0).astype(jnp.bfloat16)
            rows[q, :, FINE * jc : FINE * jc + width] = block[:, 0:width]

        put(3, result[0:64, :])
        for step in range(1, 4):
            even = result[128 * step - 64 : 128 * step, :]
            odd = result[128 * step : 128 * step + 64, :]
            put(3 + step, even - odd)
            put(3 - step, even + odd)
        copy(q).start()

    def two_rows(i, carry):
        one_row(2 * i, lhs_a, lhs_b, turn_b, turn_a)
        one_row(2 * i + 1, lhs_b, lhs_a, turn_a, turn_b)
        return carry

    turn_row(0, turn_a)
    turn_row(1, turn_b)
    rotate(0, turn_a, lhs_a)
    lax.fori_loop(0, ROWS // 2 - 1, two_rows, 0)
    one_row(ROWS - 2, lhs_a, lhs_b, turn_b, None)
    one_row(ROWS - 1, lhs_b, None, None, None)
    for q in range(ROWS):
        copy(q).wait()


def cost(flops, moved):
    return pl.CostEstimate(flops=flops, transcendentals=0, bytes_accessed=moved)


def half_of(x, first):
    def kernel(ref, out):
        out[...] = ref[first : first + QBLK // 2, :]

    return pl.pallas_call(
        kernel,
        out_shape=pltpu.VMEM((QBLK // 2, PACKED), jnp.bfloat16),
        in_specs=[pl.BlockSpec(memory_space=pltpu.VMEM)],
        out_specs=pl.BlockSpec(memory_space=pltpu.VMEM),
        compiler_params=pltpu.CompilerParams(vmem_limit_bytes=2**21),
        name="half",
    )(pltpu.with_memory_space_constraint(x, pltpu.VMEM))


def gather_pieces(x):
    def shift(v, d):
        return lax.ppermute(v, "lev", [(i, (i + d) % 8) for i in range(8)])

    p1, m1 = shift(x, 1), shift(x, -1)
    p2, m2 = shift(x, 2), shift(x, -2)
    p3, m3 = shift(p2, 1), shift(m2, -1)
    p4, m4 = shift(half_of(p2, 0), 2), shift(half_of(m2, QBLK // 2), -2)
    return x, p1, m1, p2, m2, p3, m3, p4, m4


def program(spectral, legendre, wave_pair, lat_slot):
    bf16, f32 = jnp.bfloat16, jnp.float32
    smem = pl.BlockSpec(memory_space=pltpu.SMEM)
    vmem = pl.BlockSpec(memory_space=pltpu.VMEM)
    hbm = pl.BlockSpec(memory_space=pltpu.HBM)
    z = lax.axis_index("lev").astype(jnp.int32)
    w = lax.axis_index("wav").astype(jnp.int32)
    device = w.reshape(1)
    pairs = jnp.broadcast_to(wave_pair[:, None], (KEEP // 2, 2)).reshape(1, KEEP)

    def here(v):
        return pltpu.with_memory_space_constraint(v, pltpu.VMEM)

    def params(mib):
        return pltpu.CompilerParams(vmem_limit_bytes=mib * 2**20)

    packed = pl.pallas_call(
        pack_kernel,
        out_shape=pltpu.VMEM((QBLK, PACKED), bf16),
        in_specs=[hbm], out_specs=vmem,
        scratch_shapes=[pltpu.VMEM((QBLK, 128), f32),
                        pltpu.VMEM((SLOTS, QBLK, FOLD), bf16),
                        pltpu.SemaphoreType.DMA((SLOTS,))],
        compiler_params=params(4),
        name="pack",
    )(pltpu.with_memory_space_constraint(jnp.transpose(legendre, (0, 2, 1)), pltpu.HBM))
    pieces = gather_pieces(packed)

    rhs = pl.pallas_call(
        mask_kernel,
        out_shape=pltpu.VMEM((SLOTS, KP, 256), bf16),
        in_specs=[smem, smem, vmem], out_specs=vmem,
        scratch_shapes=[pltpu.VMEM((128, 128), f32)],
        cost_estimate=cost(2_000_000_000, 2_500_000),
        compiler_params=params(6),
        name="mask",
    )(device, wave_pair, spectral)

    fine, coarse = pl.pallas_call(
        table_kernel,
        out_shape=(pltpu.HBM((ROWS, FINE, 2 * KP), bf16),
                   pltpu.HBM((ROWS, 8, 2 * KP), f32)),
        in_specs=[smem, smem, vmem], out_specs=(hbm, hbm),
        scratch_shapes=[pltpu.VMEM((1, KP), jnp.int32),
                        pltpu.VMEM((ROWS, FINE, 2 * KP), bf16),
                        pltpu.VMEM((ROWS, 8, 2 * KP), f32),
                        pltpu.SemaphoreType.DMA((2, ROWS))],
        cost_estimate=cost(4_000_000_000, 4_500_000),
        compiler_params=params(8),
        name="tables",
    )(device, lat_slot, pairs)

    near = pl.pallas_call(
        near_kernel,
        out_shape=pltpu.VMEM((32, 2 * SLOTS, ROWS, 128), bf16),
        in_specs=[smem] + [vmem] * 6, out_specs=vmem,
        cost_estimate=cost(1_000_000_000, 3_000_000),
        compiler_params=params(8),
        name="near",
    )(z.reshape(1), here(rhs), *[here(p) for p in pieces[:5]])

    fourier = pl.pallas_call(
        far_kernel,
        out_shape=pltpu.VMEM((32, 2 * SLOTS, ROWS, 128), bf16),
        in_specs=[smem, hbm] + [vmem] * 6, out_specs=vmem,
        input_output_aliases={2: 0},
        cost_estimate=cost(2 * 96 * 512 * 256 * SLOTS, 2_000_000),
        compiler_params=params(8),
        name="far",
    )(z.reshape(1), pltpu.with_memory_space_constraint(coarse, pltpu.HBM), here(near), here(rhs),
      *[here(p) for p in pieces[5:]])

    received = lax.all_to_all(fourier, "wav", split_axis=0, concat_axis=0, tiled=True)

    return pl.pallas_call(
        synth_kernel,
        out_shape=jax.ShapeDtypeStruct((ROWS, 64, WIDTH), bf16),
        in_specs=[smem, smem, vmem, vmem, vmem],
        out_specs=pl.BlockSpec(memory_space=pltpu.HBM),
        scratch_shapes=[pltpu.VMEM((KP * ROWS, 128), f32),
                        pltpu.VMEM((128, KP), f32),
                        pltpu.VMEM((128, KP), f32),
                        pltpu.VMEM((64 * COARSE, 2 * KP), bf16),
                        pltpu.VMEM((64 * COARSE, 2 * KP), bf16),
                        pltpu.VMEM((ROWS, 64, WIDTH), bf16),
                        pltpu.SemaphoreType.DMA((ROWS,))],
        cost_estimate=cost(2 * 448 * 1024 * 256 * ROWS, 18_000_000),
        compiler_params=params(16),
        name="synth",
    )(device, lat_slot, here(received.reshape(KEEP, ROWS, 128)),
      here(fine), here(coarse))


def solution(mesh):
    return jax.shard_map(
        program,
        mesh=mesh,
        in_specs=(P("wav", None, "lev"), P("wav", None, "lev"), P(), P()),
        out_specs=P("wav", "lev", None),
        check_vma=False,
    )
```
